128 devices in a mesh: dp: 1, tp: 2 (over core), wg: 64 (over z, y, x).
Axes of the slice: x: 4, y: 4, z: 4, core: 2. Of those that a mesh axis runs over, the one named last changes fastest.
Arguments:
- hidden: bfloat16 [64, 1024, 1024], P(('dp', 'wg'))
- attn_mask: int32 [64, 1024], P(('dp', 'wg'))
- ln1_scale: bfloat16 [2, 1024], replicated
- ln1_bias: bfloat16 [2, 1024], replicated
- w_qkv: bfloat16 [2, 1024, 16, 3, 64], P(None, 'wg', 'tp')
- b_qkv: bfloat16 [2, 16, 3, 64], P(None, 'tp')
- w_out: bfloat16 [2, 16, 64, 1024], P(None, 'tp', None, 'wg')
- b_out: bfloat16 [2, 1024], replicated
- ln2_scale: bfloat16 [2, 1024], replicated
- ln2_bias: bfloat16 [2, 1024], replicated
- w_up: bfloat16 [2, 1024, 4096], P(None, 'wg', 'tp')
- b_up: bfloat16 [2, 4096], P(None, 'tp')
- w_down: bfloat16 [2, 4096, 1024], P(None, 'tp', 'wg')
- b_down: bfloat16 [2, 1024], replicated
Outputs:
- output 1: bfloat16 [64, 1024, 1024], P(('dp', 'wg'))
- output 2: bfloat16 [2, 64, 1024, 16, 64], P(None, ('dp', 'wg'), None, 'tp')
- output 3: bfloat16 [2, 64, 1024, 16, 64], P(None, ('dp', 'wg'), None, 'tp')
All inputs are finite; a program needn't handle non-finite values.
Results may differ from the reference program's by a relative error of at most 0.02.
Values are sent between devices in bfloat16 or wider.
A program may use at most 1 GiB of HBM per device.

```python
import math
import jax
import jax.numpy as jnp
from jax import lax

HID = 1024
HEADS = 16
HEAD = 64
SEQ = 1024
BATCH = 64
LAYERS = 2

MIN_LEN = SEQ // 8
LN_EPS = 1e-5


def alibi_slopes(n_heads):
    closest = 2 ** int(math.floor(math.log2(n_heads)))
    slope_base = 2.0 ** (-8.0 / closest)
    slope_list = [slope_base ** (i + 1) for i in range(closest)]
    extra_base = 2.0 ** (-4.0 / closest)
    slope_list = slope_list + [extra_base ** (2 * i + 1) for i in range(n_heads - closest)]
    return jnp.array(slope_list, dtype=jnp.float32)


def layer_norm(values, ln_scale, ln_shift):
    as_float = values.astype(jnp.float32)
    mean_val = jnp.mean(as_float, axis=-1, keepdims=True)
    centered = as_float - mean_val
    variance = jnp.mean(centered * centered, axis=-1, keepdims=True)
    normed = centered * lax.rsqrt(variance + LN_EPS)
    return (normed * ln_scale.astype(jnp.float32) + ln_shift.astype(jnp.float32)).astype(jnp.bfloat16)


def decoder_layer(hidden, layer_params, positions, allowed, slopes):
    (ln1_scale, ln1_bias, w_qkv, b_qkv, w_out, b_out,
     ln2_scale, ln2_bias, w_up, b_up, w_down, b_down) = layer_params
    normed = layer_norm(hidden, ln1_scale, ln1_bias)
    qkv_out = jnp.dot(normed, w_qkv.reshape(HID, HEADS * 3 * HEAD), preferred_element_type=jnp.float32)
    qkv_out = (qkv_out + b_qkv.reshape(HEADS * 3 * HEAD).astype(jnp.float32)).astype(jnp.bfloat16)
    qkv_out = qkv_out.reshape(SEQ, HEADS, 3, HEAD)
    query_heads = qkv_out[:, :, 0]
    key_heads = qkv_out[:, :, 1]
    value_heads = qkv_out[:, :, 2]
    scores = jnp.einsum('qnd,knd->nqk', query_heads.astype(jnp.float32), key_heads.astype(jnp.float32)) / math.sqrt(HEAD)
    rel_pos = positions[None, :] - positions[:, None]
    scores = scores + slopes[:, None, None] * rel_pos[None]
    scores = jnp.where(allowed[None], scores, -1e30)
    attn_probs = jax.nn.softmax(scores, axis=-1).astype(jnp.bfloat16)
    context = jnp.einsum('nqk,knd->qnd', attn_probs.astype(jnp.float32), value_heads.astype(jnp.float32)).astype(jnp.bfloat16)
    attn_sum = jnp.dot(context.reshape(SEQ, HID), w_out.reshape(HID, HID), preferred_element_type=jnp.float32)
    mid_hidden = (hidden.astype(jnp.float32) + attn_sum + b_out.astype(jnp.float32)).astype(jnp.bfloat16)
    normed_mlp = layer_norm(mid_hidden, ln2_scale, ln2_bias)
    up_pre = jnp.dot(normed_mlp, w_up, preferred_element_type=jnp.float32) + b_up.astype(jnp.float32)
    up_act = jax.nn.gelu(up_pre, approximate=True).astype(jnp.bfloat16)
    down_sum = jnp.dot(up_act, w_down, preferred_element_type=jnp.float32)
    new_hidden = (mid_hidden.astype(jnp.float32) + down_sum + b_down.astype(jnp.float32)).astype(jnp.bfloat16)
    return new_hidden, (key_heads, value_heads)


def one_sequence(hidden, row_mask, params):
    positions = jnp.maximum(jnp.cumsum(row_mask) - 1, 0).astype(jnp.float32)
    token_idx = jnp.arange(SEQ)
    same_tok = token_idx[None, :] == token_idx[:, None]
    allowed = (token_idx[None, :] <= token_idx[:, None]) & ((row_mask[None, :] == 1) | same_tok)
    slopes = alibi_slopes(HEADS)

    def layer_step(carry_hidden, layer_params):
        return decoder_layer(carry_hidden, layer_params, positions, allowed, slopes)

    final_hidden, caches = lax.scan(layer_step, hidden, params)
    return final_hidden, caches[0], caches[1]


def setup_inputs(seed: int = 0, part: int = 0) -> dict:
    root_key = jax.random.key(seed)
    weight_keys = jax.random.split(root_key, 12)
    data_keys = jax.random.split(jax.random.fold_in(root_key, part), 3)
    hidden = jax.random.normal(data_keys[0], (BATCH, SEQ, HID), jnp.float32).astype(jnp.bfloat16)
    lengths = jax.random.randint(data_keys[1], (BATCH,), MIN_LEN, SEQ + 1)
    full_row = jax.random.randint(data_keys[2], (), 0, BATCH)
    lengths = jnp.where(jnp.arange(BATCH) == full_row, SEQ, lengths)
    attn_mask = (jnp.arange(SEQ)[None, :] >= (SEQ - lengths)[:, None]).astype(jnp.int32)

    def draw_normal(rng_key, out_shape, std_scale, offset):
        drawn = jax.random.normal(rng_key, out_shape, jnp.float32) * std_scale + offset
        return drawn.astype(jnp.bfloat16)

    return {
        'hidden': hidden,
        'attn_mask': attn_mask,
        'ln1_scale': draw_normal(weight_keys[0], (LAYERS, HID), 0.25, 1.0),
        'ln1_bias': draw_normal(weight_keys[1], (LAYERS, HID), 0.25, 0.0),
        'w_qkv': draw_normal(weight_keys[2], (LAYERS, HID, HEADS, 3, HEAD), HID ** -0.5, 0.0),
        'b_qkv': draw_normal(weight_keys[3], (LAYERS, HEADS, 3, HEAD), 0.3, 0.0),
        'w_out': draw_normal(weight_keys[4], (LAYERS, HEADS, HEAD, HID), HID ** -0.5, 0.0),
        'b_out': draw_normal(weight_keys[5], (LAYERS, HID), 0.3, 0.0),
        'ln2_scale': draw_normal(weight_keys[6], (LAYERS, HID), 0.25, 1.0),
        'ln2_bias': draw_normal(weight_keys[7], (LAYERS, HID), 0.25, 0.0),
        'w_up': draw_normal(weight_keys[8], (LAYERS, HID, 4 * HID), HID ** -0.5, 0.0),
        'b_up': draw_normal(weight_keys[9], (LAYERS, 4 * HID), 0.3, 0.0),
        'w_down': draw_normal(weight_keys[10], (LAYERS, 4 * HID, HID), (4 * HID) ** -0.5, 0.0),
        'b_down': draw_normal(weight_keys[11], (LAYERS, HID), 0.3, 0.0),
    }


def reference(hidden, attn_mask, ln1_scale, ln1_bias, w_qkv, b_qkv, w_out, b_out,
              ln2_scale, ln2_bias, w_up, b_up, w_down, b_down):
    params = (ln1_scale, ln1_bias, w_qkv, b_qkv, w_out, b_out,
              ln2_scale, ln2_bias, w_up, b_up, w_down, b_down)

    def run_sequence(seq_pair):
        return one_sequence(seq_pair[0], seq_pair[1], params)

    final_hidden, key_cache, value_cache = lax.map(run_sequence, (hidden, attn_mask))
    return final_hidden, jnp.moveaxis(key_cache, 0, 1), jnp.moveaxis(value_cache, 0, 1)
```

```python
import math
import jax
import jax.numpy as jnp
from jax import lax
from jax.experimental import pallas as pl
from jax.experimental.pallas import tpu as pltpu
from jax.sharding import PartitionSpec as P

LN_EPS = 1e-5
MESH = pl.DeviceIdType.MESH
UNITS = 24
CHUNKS = 16
STAGES = 6
ORDERS = (('x', 'y', 'z'), ('y', 'z', 'x'), ('z', 'x', 'y'))


def alibi_slopes(n_heads):
    closest = 2 ** int(math.floor(math.log2(n_heads)))
    slope_base = 2.0 ** (-8.0 / closest)
    slope_list = [slope_base ** (i + 1) for i in range(closest)]
    extra_base = 2.0 ** (-4.0 / closest)
    slope_list = slope_list + [extra_base ** (2 * i + 1) for i in range(n_heads - closest)]
    return jnp.array(slope_list, dtype=jnp.float32)


def layer_norm(values, ln_scale, ln_shift):
    as_float = values.astype(jnp.float32)
    mean_val = jnp.mean(as_float, axis=-1, keepdims=True)
    centered = as_float - mean_val
    variance = jnp.mean(centered * centered, axis=-1, keepdims=True)
    normed = centered * lax.rsqrt(variance + LN_EPS)
    return (normed * ln_scale.astype(jnp.float32) + ln_shift.astype(jnp.float32)).astype(jnp.bfloat16)


def add_residual(hidden, branch, bias):
    return (hidden.astype(jnp.float32) + branch.astype(jnp.float32) + bias.astype(jnp.float32)).astype(jnp.bfloat16)


def alibi_attention(query_heads, key_heads, value_heads, attn_mask, slopes):
    seq_len = query_heads.shape[1]
    head_dim = query_heads.shape[-1]
    positions = jnp.maximum(jnp.cumsum(attn_mask, axis=1) - 1, 0).astype(jnp.float32)
    token_idx = jnp.arange(seq_len)
    causal = token_idx[None, :] <= token_idx[:, None]
    same_tok = token_idx[None, :] == token_idx[:, None]
    allowed = causal[None] & ((attn_mask[:, None, :] == 1) | same_tok[None])
    scores = jnp.einsum('bqnd,bknd->bnqk', query_heads, key_heads, preferred_element_type=jnp.float32) / math.sqrt(head_dim)
    rel_pos = positions[:, None, :] - positions[:, :, None]
    scores = scores + slopes[None, :, None, None] * rel_pos[:, None]
    scores = jnp.where(allowed[:, None], scores, -1e30)
    attn_probs = jax.nn.softmax(scores, axis=-1).astype(jnp.bfloat16)
    return jnp.einsum('bnqk,bknd->bqnd', attn_probs, value_heads, preferred_element_type=jnp.float32).astype(jnp.bfloat16)


class Torus:
    def __init__(self, blocks, send_sem, recv_sem):
        self.blocks, self.send_sem, self.recv_sem = blocks, send_sem, recv_sem
        me = lax.axis_index('wg')
        self.pos = {'z': lax.div(me, 16), 'y': lax.rem(lax.div(me, 4), 4), 'x': lax.rem(me, 4)}
        self.next = {ax: lax.rem(p + 1, 4) for ax, p in self.pos.items()}
        self.prev = {ax: lax.rem(p + 3, 4) for ax, p in self.pos.items()}
        self.right = {ax: self.device({**self.pos, ax: self.next[ax]}) for ax in 'zyx'}
        self.left = {ax: self.device({**self.pos, ax: self.prev[ax]}) for ax in 'zyx'}

    @staticmethod
    def device(pos):
        return pos['z'] * 16 + pos['y'] * 4 + pos['x']

    def view(self, unit, where, cols=None):
        ref = self.blocks.at[unit, where['z'], where['y'], where['x']]
        return ref if cols is None else self.blocks.at[unit, where['z'], where['y'], where['x'], :, cols]

    def barrier(self):
        sem = pltpu.get_barrier_semaphore()
        for ax in 'zyx':
            for dev in (self.left[ax], self.right[ax]):
                pl.semaphore_signal(sem, inc=1, device_id={'wg': dev}, device_id_type=MESH)
        pl.semaphore_wait(sem, 6)

    def sends(self, chunk, stage):
        every, low, high = slice(None), slice(0, 2), slice(2, 4)
        out = []
        for color, (a, b, c) in enumerate(ORDERS):
            unit = 3 * chunk + color
            if stage == 0:
                here = dict(self.pos)
                out += [(self.view(unit, here), self.right[a]), (self.view(unit, here), self.left[a])]
            elif stage == 1:
                out += [(self.view(unit, {**self.pos, a: self.prev[a]}, slice(0, 128)), self.right[a]),
                        (self.view(unit, {**self.pos, a: self.next[a]}, slice(128, 256)), self.left[a])]
            elif stage == 2:
                row = {**self.pos, a: every}
                out += [(self.view(unit, row), self.right[b]), (self.view(unit, row), self.left[b])]
            elif stage == 3:
                out += [(self.view(unit, {a: low, b: self.prev[b], c: self.pos[c]}), self.right[b]),
                        (self.view(unit, {a: high, b: self.next[b], c: self.pos[c]}), self.left[b])]
            elif stage == 4:
                plane = {a: every, b: every, c: self.pos[c]}
                out += [(self.view(unit, plane), self.right[c]), (self.view(unit, plane), self.left[c])]
            else:
                slow, fast = (a, b) if 'zyx'.index(a) < 'zyx'.index(b) else (b, a)
                out += [(self.view(unit, {slow: low, fast: every, c: self.prev[c]}), self.right[c]),
                        (self.view(unit, {slow: high, fast: every, c: self.next[c]}), self.left[c])]
        return out

    def start(self, chunk, stage):
        for ref, dev in self.sends(chunk, stage):
            pltpu.make_async_remote_copy(
                src_ref=ref, dst_ref=ref, send_sem=self.send_sem.at[chunk, stage], recv_sem=self.recv_sem.at[chunk, stage],
                device_id={'wg': dev}, device_id_type=MESH).start()

    def wait(self, sem, chunk, stage):
        w = self.blocks
        size = (w.at[0:3, 0, 0, 0:2], w.at[0:3, 0, 0, 0], w.at[0:3, 0, 0:2], w.at[0:3, 0, 0], w.at[0:3, 0:2], w.at[0:3, 0])[stage]
        pltpu.make_async_copy(size, size, sem.at[chunk, stage]).wait()

    def step(self, chunk, stage):
        if stage > 0:
            self.wait(self.recv_sem, chunk, stage - 1)
        if stage < STAGES:
            self.start(chunk, stage)


def gather_kernel(local_ref, blocks, send_sem, recv_sem, own_sem):
    torus = Torus(blocks, send_sem, recv_sem)
    own = pltpu.make_async_copy(local_ref, blocks.at[:, torus.pos['z'], torus.pos['y'], torus.pos['x']], own_sem)
    own.start()
    torus.barrier()
    own.wait()
    spacing = 2

    def tick(t, carry):
        for stage in reversed(range(STAGES + 1)):
            chunk = t - spacing * stage

            @pl.when((chunk >= 0) & (chunk < CHUNKS))
            def _():
                torus.step(chunk, stage)
        return carry

    lax.fori_loop(0, CHUNKS + spacing * STAGES, tick, 0)

    def drain(chunk, carry):
        for stage in range(STAGES):
            torus.wait(send_sem, chunk, stage)
        return carry

    lax.fori_loop(0, CHUNKS, drain, 0)


def gather_weights(local):
    return pl.pallas_call(
        gather_kernel,
        out_shape=jax.ShapeDtypeStruct((2 * UNITS, 4, 4, 4, 16, 256), jnp.bfloat16),
        in_specs=[pl.BlockSpec(memory_space=pl.ANY)],
        out_specs=pl.BlockSpec(memory_space=pl.ANY),
        scratch_shapes=[
            pltpu.SemaphoreType.DMA((CHUNKS, STAGES)),
            pltpu.SemaphoreType.DMA((CHUNKS, STAGES)),
            pltpu.SemaphoreType.DMA,
        ],
        compiler_params=pltpu.CompilerParams(collective_id=0, has_side_effects=True),
        name='torus_gather',
    )(local)


def pack_local(w_qkv, w_out, w_up, w_down):
    def units(w):
        return w.reshape(w.shape[0], 16, -1, 256).transpose(0, 2, 1, 3)
    qkv = units(w_qkv.transpose(0, 1, 3, 2, 4))
    out = units(w_out.reshape(w_out.shape[0], -1, 16).transpose(0, 2, 1))
    up = units(w_up)
    down = units(w_down.transpose(0, 2, 1))
    return jnp.concatenate([qkv, out, up, down], axis=1).reshape(-1, 16, 256)


def solution(mesh):
    tp_size = mesh.shape['tp']
    batch_axes = ('dp', 'wg')

    def device_fn(hidden, attn_mask, ln1_scale, ln1_bias, w_qkv, b_qkv, w_out, b_out,
                  ln2_scale, ln2_bias, w_up, b_up, w_down, b_down):
        local_heads = w_qkv.shape[2]
        head_start = lax.axis_index('tp') * local_heads
        slopes = lax.dynamic_slice_in_dim(alibi_slopes(local_heads * tp_size), head_start, local_heads)
        blocks = gather_weights(pack_local(w_qkv, w_out, w_up, w_down)).reshape(2, UNITS, 1024, 256)
        key_list = []
        value_list = []
        for layer_idx in range(w_qkv.shape[0]):
            w = blocks[layer_idx]
            normed = layer_norm(hidden, ln1_scale[layer_idx], ln1_bias[layer_idx])
            qkv_out = jnp.einsum('bsh,uhc->bsuc', normed, w[0:6], preferred_element_type=jnp.float32)
            qkv_out = qkv_out.reshape(1, 1024, 3, local_heads, 64)
            qkv_out = (qkv_out + b_qkv[layer_idx].transpose(1, 0, 2).astype(jnp.float32)).astype(jnp.bfloat16)
            key_heads, value_heads = qkv_out[:, :, 1], qkv_out[:, :, 2]
            context = alibi_attention(qkv_out[:, :, 0], key_heads, value_heads, attn_mask, slopes)
            attn_part = jnp.einsum('bsuc,uhc->bsh', context.reshape(1, 1024, 2, 256), w[6:8], preferred_element_type=jnp.float32).astype(jnp.bfloat16)
            attn_sum = lax.psum(attn_part, 'tp')
            mid_hidden = add_residual(hidden, attn_sum, b_out[layer_idx])
            normed_mlp = layer_norm(mid_hidden, ln2_scale[layer_idx], ln2_bias[layer_idx])
            up_pre = jnp.einsum('bsh,uhc->bsuc', normed_mlp, w[8:16], preferred_element_type=jnp.float32)
            up_act = jax.nn.gelu(up_pre + b_up[layer_idx].reshape(8, 256).astype(jnp.float32), approximate=True).astype(jnp.bfloat16)
            down_part = jnp.einsum('bsuc,uhc->bsh', up_act, w[16:24], preferred_element_type=jnp.float32).astype(jnp.bfloat16)
            down_sum = lax.psum(down_part, 'tp')
            hidden = add_residual(mid_hidden, down_sum, b_down[layer_idx])
            key_list.append(key_heads)
            value_list.append(value_heads)
        return hidden, jnp.stack(key_list), jnp.stack(value_list)

    replicated = P(None, None)
    in_specs = (P(batch_axes, None, None), P(batch_axes, None), replicated, replicated,
                P(None, 'wg', 'tp', None, None), P(None, 'tp', None, None), P(None, 'tp', None, 'wg'), replicated,
                replicated, replicated, P(None, 'wg', 'tp'), P(None, 'tp'), P(None, 'tp', 'wg'), replicated)
    cache_spec = P(None, batch_axes, None, 'tp', None)
    out_specs = (P(batch_axes, None, None), cache_spec, cache_spec)
    return jax.shard_map(device_fn, mesh=mesh, in_specs=in_specs, out_specs=out_specs, check_vma=False)
```

```python
import math
import jax
import jax.numpy as jnp
from jax import lax
from jax.experimental import pallas as pl
from jax.experimental.pallas import tpu as pltpu
from jax.sharding import PartitionSpec as P

LN_EPS = 1e-5
MESH = pl.DeviceIdType.MESH
UNITS = 24
CHUNKS = 16
STAGES = 6
OFFSETS = (0, 1, 4, 5, 8, 10, 12)
HEAD_TICKS = 15
LAYER_TICKS = 14
NT = (((1,), (1,)), ((), ()))
ORDERS = (('x', 'y', 'z'), ('y', 'z', 'x'), ('z', 'x', 'y'))


def alibi_slopes(n_heads):
    closest = 2 ** int(math.floor(math.log2(n_heads)))
    slope_base = 2.0 ** (-8.0 / closest)
    slope_list = [slope_base ** (i + 1) for i in range(closest)]
    extra_base = 2.0 ** (-4.0 / closest)
    slope_list = slope_list + [extra_base ** (2 * i + 1) for i in range(n_heads - closest)]
    return jnp.array(slope_list, dtype=jnp.float32)


class Torus:
    def __init__(self, blocks, send_sem, recv_sem):
        self.blocks, self.send_sem, self.recv_sem = blocks, send_sem, recv_sem
        me = lax.axis_index('wg')
        self.pos = {'z': lax.div(me, 16), 'y': lax.rem(lax.div(me, 4), 4), 'x': lax.rem(me, 4)}
        self.next = {ax: lax.rem(p + 1, 4) for ax, p in self.pos.items()}
        self.prev = {ax: lax.rem(p + 3, 4) for ax, p in self.pos.items()}
        self.right = {ax: self.device({**self.pos, ax: self.next[ax]}) for ax in 'zyx'}
        self.left = {ax: self.device({**self.pos, ax: self.prev[ax]}) for ax in 'zyx'}

    @staticmethod
    def device(pos):
        return pos['z'] * 16 + pos['y'] * 4 + pos['x']

    def view(self, unit, where, cols=None):
        ref = self.blocks.at[unit, where['z'], where['y'], where['x']]
        return ref if cols is None else self.blocks.at[unit, where['z'], where['y'], where['x'], :, cols]

    def barrier(self):
        sem = pltpu.get_barrier_semaphore()
        for ax in 'zyx':
            for dev in (self.left[ax], self.right[ax]):
                pl.semaphore_signal(sem, inc=1, device_id={'wg': dev}, device_id_type=MESH)
        pl.semaphore_signal(sem, inc=1, device_id={'tp': 1 - lax.axis_index('tp')}, device_id_type=MESH)
        pl.semaphore_wait(sem, 7)

    def sends(self, chunk, stage):
        every, low, high = slice(None), slice(0, 2), slice(2, 4)
        out = []
        for color, (a, b, c) in enumerate(ORDERS):
            unit = 3 * chunk + color
            if stage == 0:
                here = dict(self.pos)
                out += [(self.view(unit, here), self.right[a]), (self.view(unit, here), self.left[a])]
            elif stage == 1:
                out += [(self.view(unit, {**self.pos, a: self.prev[a]}, slice(0, 128)), self.right[a]),
                        (self.view(unit, {**self.pos, a: self.next[a]}, slice(128, 256)), self.left[a])]
            elif stage == 2:
                row = {**self.pos, a: every}
                out += [(self.view(unit, row), self.right[b]), (self.view(unit, row), self.left[b])]
            elif stage == 3:
                out += [(self.view(unit, {a: low, b: self.prev[b], c: self.pos[c]}), self.right[b]),
                        (self.view(unit, {a: high, b: self.next[b], c: self.pos[c]}), self.left[b])]
            elif stage == 4:
                plane = {a: every, b: every, c: self.pos[c]}
                out += [(self.view(unit, plane), self.right[c]), (self.view(unit, plane), self.left[c])]
            else:
                slow, fast = (a, b) if 'zyx'.index(a) < 'zyx'.index(b) else (b, a)
                out += [(self.view(unit, {slow: low, fast: every, c: self.prev[c]}), self.right[c]),
                        (self.view(unit, {slow: high, fast: every, c: self.next[c]}), self.left[c])]
        return out

    def start(self, chunk, stage):
        for ref, dev in self.sends(chunk, stage):
            pltpu.make_async_remote_copy(
                src_ref=ref, dst_ref=ref, send_sem=self.send_sem.at[chunk, stage], recv_sem=self.recv_sem.at[chunk, stage],
                device_id={'wg': dev}, device_id_type=MESH).start()

    def wait(self, sem, chunk, stage):
        w = self.blocks
        size = (w.at[0:3, 0, 0, 0:2], w.at[0:3, 0, 0, 0], w.at[0:3, 0, 0:2], w.at[0:3, 0, 0], w.at[0:3, 0:2], w.at[0:3, 0])[stage]
        pltpu.make_async_copy(size, size, sem.at[chunk, stage]).wait()

    def step(self, chunk, stage):
        if stage > 0:
            self.wait(self.recv_sem, chunk, stage - 1)
        if stage < STAGES:
            self.start(chunk, stage)

    def tick(self, t, odd):
        for stage in ((1, 3) if odd else (4, 5, 2, 0, 6)):
            chunk = lax.div(t - OFFSETS[stage], 2)

            @pl.when((t >= OFFSETS[stage]) & (chunk < CHUNKS))
            def _():
                self.step(chunk, stage)


def normalize(values, scale, shift):
    mean = jnp.mean(values, axis=1, keepdims=True)
    centered = values - mean
    variance = jnp.mean(centered * centered, axis=1, keepdims=True)
    return (centered * lax.rsqrt(variance + LN_EPS) * scale + shift).astype(jnp.bfloat16)


def rows(r, size=256):
    return pl.ds(pl.multiple_of(r * size, size), size)


def layers_kernel(x_hbm, mask_ref, slope_ref, ln1s_ref, ln1b_ref, ln2s_ref, ln2b_ref, bqkv_ref, bout_ref, bup_ref, bdown_ref,
                  local_ref, out_hbm, cache_hbm,
                  blocks, x, a, qkv, ctx, act, acc, part, other, bias_cols, limits,
                  send_sem, recv_sem, part_send, part_recv, own_sem, x_sem, cache_sem, out_sem):
    f32, bf16 = jnp.float32, jnp.bfloat16
    torus = Torus(blocks, send_sem, recv_sem)
    partner = {'tp': 1 - lax.axis_index('tp')}
    own = pltpu.make_async_copy(local_ref, blocks.at[:, torus.pos['z'], torus.pos['y'], torus.pos['x']], own_sem)
    own.start()
    x_in = pltpu.make_async_copy(x_hbm, x, x_sem)
    x_in.start()
    torus.barrier()
    own.wait()
    torus.tick(jnp.int32(0), False)

    def row_of(ref, layer):
        both = ref[...].astype(f32)
        return jnp.where(layer == 0, both[0:1], both[1:2])

    def weight(unit):
        return blocks[unit].reshape(1024, 256)

    real = jnp.sum(mask_ref[...].astype(f32), axis=1, keepdims=True)
    key = lax.broadcasted_iota(jnp.int32, (1024, 128), 0).astype(f32)
    lane = lax.broadcasted_iota(jnp.int32, (1024, 128), 1)
    place = key - (1024.0 - real)
    slope = jnp.where(lax.axis_index('tp') == 0, slope_ref[0:1], slope_ref[1:2])
    key_bias = jnp.where(place >= 0.0, place * slope, -1e30)
    first = key_bias.astype(bf16)
    rest = key_bias - first.astype(f32)
    second = rest.astype(bf16)
    third = (rest - second.astype(f32)).astype(bf16)
    which = lax.rem(lane, 3)
    split = jnp.where(which == 0, first.astype(f32), jnp.where(which == 1, second.astype(f32), third.astype(f32)))
    bias_cols[...] = jnp.where(lane < 24, split, 0.0).astype(bf16)
    row = lax.broadcasted_iota(jnp.int32, (256, 256), 0)
    col = lax.broadcasted_iota(jnp.int32, (256, 256), 1)
    limits[0] = jnp.where(col <= row, 3e38, -1e30)
    limits[1] = jnp.where(col == row, -1e29, -3e38)

    x_in.wait()

    def first_norm(r, carry):
        a[rows(r)] = normalize(x[rows(r)].astype(f32), ln1s_ref[0:1].astype(f32), ln1b_ref[0:1].astype(f32))
        return carry

    lax.fori_loop(0, 4, first_norm, 0)

    def head_tick(i, carry):
        torus.tick(2 * i + 1, True)
        torus.tick(2 * i + 2, False)
        return carry

    lax.fori_loop(0, (HEAD_TICKS - 1) // 2, head_tick, 0)

    def exchange(layer, kind, r):
        view = lambda ref: ref.at[kind, rows(r)]
        return pltpu.make_async_remote_copy(
            src_ref=view(part), dst_ref=view(other), send_sem=part_send.at[layer, kind, r], recv_sem=part_recv.at[layer, kind, r],
            device_id=partner, device_id_type=MESH)

    def residual(layer, kind, r, bias):
        exchange(layer, kind, r).wait_recv()
        branch = part[kind, rows(r)].astype(f32) + other[kind, rows(r)].astype(f32)
        total = (x[rows(r)].astype(f32) + branch + bias).astype(bf16)
        x[rows(r)] = total
        return total.astype(f32)

    def attention(pair, carry):
        unit, lanes = lax.div(pair, 2), pl.ds(pl.multiple_of(lax.rem(pair, 2) * 128, 128), 128)
        lane = lax.broadcasted_iota(jnp.int32, (256, 128), 1)
        for r in range(4):
            n = (r + 1) * 256
            q = qkv[unit, r * 256:n, lanes]
            k = jnp.concatenate([qkv[2 + unit, 0:n, lanes], bias_cols[0:n]], axis=1)
            v = jnp.concatenate([qkv[4 + unit, 0:n, lanes], jnp.ones((n, 128), bf16)], axis=1)
            outs = []
            for half in range(2):
                mine = (lane < 64) if half == 0 else (lane >= 64)
                head = 2 * pair + half
                pick = ((lane >= 3 * head) & (lane < 3 * head + 3)).astype(bf16)
                query = jnp.concatenate([jnp.where(mine, q, jnp.zeros_like(q)), pick], axis=1)
                scores = lax.dot_general(query, k, NT, preferred_element_type=f32)
                last = jnp.maximum(jnp.minimum(scores[:, r * 256:], limits[0]), limits[1])
                scores = jnp.concatenate([scores[:, :r * 256], last], axis=1) if r else last
                probs = jnp.exp(scores - jnp.max(scores, axis=1, keepdims=True)).astype(bf16)
                out = jnp.dot(probs, v, preferred_element_type=f32)
                outs.append(out[:, :128] / out[:, 128:])
            ctx[unit, r * 256:n, lanes] = jnp.where(lane < 64, outs[0], outs[1]).astype(bf16)
        return carry

    def layer_body(layer, carry):
        base = layer * UNITS
        t0 = HEAD_TICKS + layer * LAYER_TICKS

        def qkv_unit(j, carry):
            scale = jnp.where(j < 2, 0.125, 1.0)
            cols = pl.ds(pl.multiple_of(j * 256, 256), 256)
            both = bqkv_ref[:, cols].astype(f32)
            bias = jnp.where(layer == 0, both[0:1], both[1:2])
            out = jnp.dot(a[...], weight(base + j), preferred_element_type=f32) + bias
            qkv[j] = (out * scale).astype(bf16)
            return carry

        lax.fori_loop(0, 3, qkv_unit, 0)
        torus.tick(t0, True)
        torus.tick(t0 + 1, False)
        lax.fori_loop(3, 6, qkv_unit, 0)
        cache = pltpu.make_async_copy(qkv.at[2:6], cache_hbm.at[layer], cache_sem)
        cache.start()

        def attend_pair(pair, carry):
            t = t0 + 2 + pair

            @pl.when(lax.rem(pair, 2) == 0)
            def _():
                torus.tick(t, True)

            @pl.when(lax.rem(pair, 2) == 1)
            def _():
                torus.tick(t, False)

            return attention(pair, carry)

        lax.fori_loop(0, 4, attend_pair, 0)

        def send_after(kind, r):
            @pl.when(r > 0)
            def _():
                exchange(layer, kind, r - 1).start()

        def project(r, carry):
            c = jnp.concatenate([ctx[0, rows(r)], ctx[1, rows(r)]], axis=1)
            w = jnp.concatenate([weight(base + 6), weight(base + 7)], axis=1)
            part[0, rows(r)] = lax.dot_general(c, w, NT, preferred_element_type=f32).astype(bf16)
            send_after(0, r)
            return carry

        lax.fori_loop(0, 4, project, 0)
        torus.tick(t0 + 6, True)
        exchange(layer, 0, 3).start()

        def second_norm(r, carry):
            total = residual(layer, 0, r, row_of(bout_ref, layer))
            a[rows(r)] = normalize(total, row_of(ln2s_ref, layer), row_of(ln2b_ref, layer))
            return carry

        lax.fori_loop(0, 4, second_norm, 0)
        torus.tick(t0 + 7, False)

        def up_unit(j, carry):
            cols = pl.ds(pl.multiple_of(j * 256, 256), 256)
            both = bup_ref[:, cols].astype(f32)
            bias = jnp.where(layer == 0, both[0:1], both[1:2])
            out = jnp.dot(a[...], weight(base + 8 + j), preferred_element_type=f32) + bias
            act[j] = jax.nn.gelu(out, approximate=True).astype(bf16)
            return carry

        lax.fori_loop(0, 4, up_unit, 0)
        torus.tick(t0 + 8, True)
        torus.tick(t0 + 9, False)
        lax.fori_loop(4, 8, up_unit, 0)

        def down_product(r, units):
            h = jnp.concatenate([act[j, rows(r)] for j in units], axis=1)
            w = jnp.concatenate([weight(base + 16 + j) for j in units], axis=1)
            return lax.dot_general(h, w, NT, preferred_element_type=f32)

        def down_first(r, carry):
            acc[rows(r)] = down_product(r, (0, 1))
            return carry

        def down_next(r, carry):
            acc[rows(r)] += down_product(r, (2, 3, 4))
            return carry

        def down_last(r, carry):
            part[1, rows(r)] = (acc[rows(r)] + down_product(r, (5, 6, 7))).astype(bf16)
            send_after(1, r)
            return carry

        lax.fori_loop(0, 4, down_first, 0)
        torus.tick(t0 + 10, True)
        torus.tick(t0 + 11, False)
        lax.fori_loop(0, 4, down_next, 0)
        torus.tick(t0 + 12, True)
        torus.tick(t0 + 13, False)
        lax.fori_loop(0, 4, down_last, 0)
        cache.wait()
        exchange(layer, 1, 3).start()

        def finish(r, carry):
            total = residual(layer, 1, r, row_of(bdown_ref, layer))

            @pl.when(layer == 0)
            def _():
                a[rows(r)] = normalize(total, ln1s_ref[1:2].astype(f32), ln1b_ref[1:2].astype(f32))
            return carry

        lax.fori_loop(0, 4, finish, 0)

        def sent(r, carry):
            exchange(layer, 0, r).wait_send()
            exchange(layer, 1, r).wait_send()
            return carry

        lax.fori_loop(0, 4, sent, 0)
        return carry

    lax.fori_loop(0, 2, layer_body, 0)
    out = pltpu.make_async_copy(x, out_hbm, out_sem)
    out.start()

    def drain(chunk, carry):
        for stage in range(STAGES):
            torus.wait(send_sem, chunk, stage)
        return carry

    lax.fori_loop(0, CHUNKS, drain, 0)
    out.wait()


def run_layers(*operands):
    vmem, hbm = pl.BlockSpec(memory_space=pltpu.VMEM), pl.BlockSpec(memory_space=pl.ANY)
    bf16, dma = jnp.bfloat16, pltpu.SemaphoreType.DMA
    return pl.pallas_call(
        layers_kernel,
        out_shape=(jax.ShapeDtypeStruct((1024, 1024), bf16), jax.ShapeDtypeStruct((2, 4, 1024, 256), bf16)),
        in_specs=[hbm] + [vmem] * 10 + [hbm],
        out_specs=(hbm, hbm),
        scratch_shapes=[
            pltpu.VMEM((2 * UNITS, 4, 4, 4, 16, 256), bf16),
            pltpu.VMEM((1024, 1024), bf16),
            pltpu.VMEM((1024, 1024), bf16),
            pltpu.VMEM((6, 1024, 256), bf16),
            pltpu.VMEM((2, 1024, 256), bf16),
            pltpu.VMEM((8, 1024, 256), bf16),
            pltpu.VMEM((1024, 1024), jnp.float32),
            pltpu.VMEM((2, 1024, 1024), bf16),
            pltpu.VMEM((2, 1024, 1024), bf16),
            pltpu.VMEM((1024, 128), bf16),
            pltpu.VMEM((2, 256, 256), jnp.float32),
            dma((CHUNKS, STAGES)),
            dma((CHUNKS, STAGES)),
            dma((2, 2, 4)),
            dma((2, 2, 4)),
            dma,
            dma,
            dma,
            dma,
        ],
        compiler_params=pltpu.CompilerParams(collective_id=0, has_side_effects=True, vmem_limit_bytes=67043328),
        name='two_layers',
    )(*operands)


def pack_local(w_qkv, w_out, w_up, w_down):
    def units(w):
        return w.reshape(w.shape[0], 16, -1, 256).transpose(0, 2, 1, 3)
    qkv = units(w_qkv.transpose(0, 1, 3, 2, 4))
    out = units(w_out.reshape(w_out.shape[0], -1, 16).transpose(0, 2, 1))
    up = units(w_up)
    down = units(w_down.transpose(0, 2, 1))
    return jnp.concatenate([qkv, out, up, down], axis=1).reshape(-1, 16, 256)


def solution(mesh):
    tp_size = mesh.shape['tp']
    batch_axes = ('dp', 'wg')

    def device_fn(hidden, attn_mask, ln1_scale, ln1_bias, w_qkv, b_qkv, w_out, b_out,
                  ln2_scale, ln2_bias, w_up, b_up, w_down, b_down):
        n_layers, _, local_heads, _, head_dim = w_qkv.shape
        slopes = jnp.repeat(alibi_slopes(local_heads * tp_size).reshape(tp_size, local_heads), 3, axis=1)
        slopes = jnp.pad(slopes, ((0, 0), (0, 128 - slopes.shape[1])))
        out, cache = run_layers(
            hidden.reshape(hidden.shape[1:]), attn_mask, slopes, ln1_scale, ln1_bias, ln2_scale, ln2_bias,
            b_qkv.transpose(0, 2, 1, 3).reshape(n_layers, -1), b_out, b_up, b_down,
            pack_local(w_qkv, w_out, w_up, w_down))
        cache = cache.reshape(n_layers, 2, 2, 1024, 256).transpose(1, 0, 3, 2, 4)
        cache = cache.reshape(2, n_layers, 1, 1024, local_heads, head_dim)
        return out.reshape(hidden.shape), cache[0], cache[1]

    replicated = P(None, None)
    in_specs = (P(batch_axes, None, None), P(batch_axes, None), replicated, replicated,
                P(None, 'wg', 'tp', None, None), P(None, 'tp', None, None), P(None, 'tp', None, 'wg'), replicated,
                replicated, replicated, P(None, 'wg', 'tp'), P(None, 'tp'), P(None, 'tp', 'wg'), replicated)
    cache_spec = P(None, batch_axes, None, 'tp', None)
    out_specs = (P(batch_axes, None, None), cache_spec, cache_spec)
    return jax.shard_map(device_fn, mesh=mesh, in_specs=in_specs, out_specs=out_specs, check_vma=False)
```

```python
import math
import jax
import jax.numpy as jnp
import numpy as np
from jax import lax
from jax.experimental import pallas as pl
from jax.experimental.pallas import tpu as pltpu
from jax.sharding import PartitionSpec as P

LN_EPS = 1e-5
MESH = pl.DeviceIdType.MESH
UNITS = 24
CHUNKS = 16
STAGES = 6
SCHEDULE = {
    'head': ((0, 0, ((0, 0), (1, 0), (2, 0), (3, 0), (4, 0), (5, 0), (6, 0), (7, 0), (8, 0), (9, 0), (10, 0), (11, 0), (12, 0), (13, 0), (14, 0), (15, 0))),),
    'norm': ((0, 1, ((0, 1),)), (0, 2, ((1, 1), (2, 1), (3, 1), (4, 1), (5, 1))), (0, 3, ((6, 1), (7, 1), (8, 1), (9, 1)))),
    'qkv': ((0, 0, ((0, 2), (1, 2), (2, 2), (3, 2), (4, 2), (0, 3), (5, 2), (1, 3), (2, 3), (3, 3), (4, 3), (0, 4), (5, 3), (1, 4), (0, 5), (2, 4), (1, 5), (0, 6))), (0, 1, ((3, 4),)), (0, 3, ((4, 4), (1, 6))), (0, 5, ((2, 5),)), (1, 0, ((10, 4), (8, 6))), (1, 3, ((11, 4), (9, 6))), (1, 5, ((12, 3),))),
    'attn': ((0, 0, ((5, 4),)), (0, 1, ((3, 5),)), (0, 2, ((4, 5), (6, 2), (7, 2))), (0, 3, ((5, 5), (8, 2), (9, 2))), (1, 0, ((13, 3), (14, 3), (15, 3))), (1, 1, ((10, 5),)), (1, 2, ((11, 5), (12, 4))), (1, 3, ((13, 4),))),
    'proj': ((0, 0, ((2, 6), (6, 3), (10, 1), (11, 1))), (0, 1, ((7, 3), (12, 1), (13, 1), (14, 1))), (0, 2, ((15, 1),)), (1, 0, ((10, 6),)), (1, 1, ((14, 4),))),
    'mid': ((0, 1, ((6, 4),)), (0, 3, ((7, 4),)), (1, 1, ((12, 5),)), (1, 3, ((13, 5),))),
    'up': ((0, 1, ((3, 6),)), (0, 2, ((8, 3),)), (0, 3, ((9, 3), (10, 2))), (0, 4, ((4, 6), (6, 5))), (0, 5, ((11, 2),)), (0, 6, ((7, 5),)), (0, 7, ((5, 6), (8, 4))), (1, 0, ((15, 4),)), (1, 1, ((11, 6),)), (1, 3, ((14, 5),)), (1, 4, ((12, 6),)), (1, 7, ((13, 6),))),
    'd1': ((0, 0, ((6, 6), (9, 4))), (1, 0, ((14, 6),))),
    'd2': ((0, 0, ((7, 6),)), (0, 1, ((10, 3), (11, 3), (12, 2))), (0, 2, ((8, 5),)), (1, 0, ((15, 6),))),
    'fin': ((0, 0, ((13, 2), (14, 2), (15, 2))), (0, 1, ((9, 5),))),
    'd0': ((1, 0, ((15, 5),)),),
}
NT = (((1,), (1,)), ((), ()))
ORDERS = (('x', 'y', 'z'), ('y', 'z', 'x'), ('z', 'x', 'y'))


def alibi_slopes(n_heads):
    closest = 2 ** int(math.floor(math.log2(n_heads)))
    slope_base = 2.0 ** (-8.0 / closest)
    slope_list = [slope_base ** (i + 1) for i in range(closest)]
    extra_base = 2.0 ** (-4.0 / closest)
    slope_list = slope_list + [extra_base ** (2 * i + 1) for i in range(n_heads - closest)]
    return np.array(slope_list, dtype=np.float32)


class Torus:
    def __init__(self, blocks, send_sem, recv_sem):
        self.blocks, self.send_sem, self.recv_sem = blocks, send_sem, recv_sem
        me = lax.axis_index('wg')
        self.pos = {'z': lax.div(me, 16), 'y': lax.rem(lax.div(me, 4), 4), 'x': lax.rem(me, 4)}
        self.next = {ax: lax.rem(p + 1, 4) for ax, p in self.pos.items()}
        self.prev = {ax: lax.rem(p + 3, 4) for ax, p in self.pos.items()}
        self.right = {ax: self.device({**self.pos, ax: self.next[ax]}) for ax in 'zyx'}
        self.left = {ax: self.device({**self.pos, ax: self.prev[ax]}) for ax in 'zyx'}

    @staticmethod
    def device(pos):
        return pos['z'] * 16 + pos['y'] * 4 + pos['x']

    def view(self, unit, where, cols=None):
        ref = self.blocks.at[unit, where['z'], where['y'], where['x']]
        return ref if cols is None else self.blocks.at[unit, where['z'], where['y'], where['x'], :, cols]

    def barrier(self):
        sem = pltpu.get_barrier_semaphore()
        for ax in 'zyx':
            for dev in (self.left[ax], self.right[ax]):
                pl.semaphore_signal(sem, inc=1, device_id={'wg': dev}, device_id_type=MESH)
        pl.semaphore_signal(sem, inc=1, device_id={'tp': 1 - lax.axis_index('tp')}, device_id_type=MESH)
        pl.semaphore_wait(sem, 7)

    def sends(self, chunk, stage):
        every, low, high = slice(None), slice(0, 2), slice(2, 4)
        out = []
        for color, (a, b, c) in enumerate(ORDERS):
            unit = 3 * chunk + color
            if stage == 0:
                here = dict(self.pos)
                out += [(self.view(unit, here), self.right[a]), (self.view(unit, here), self.left[a])]
            elif stage == 1:
                out += [(self.view(unit, {**self.pos, a: self.prev[a]}, slice(0, 128)), self.right[a]),
                        (self.view(unit, {**self.pos, a: self.next[a]}, slice(128, 256)), self.left[a])]
            elif stage == 2:
                row = {**self.pos, a: every}
                out += [(self.view(unit, row), self.right[b]), (self.view(unit, row), self.left[b])]
            elif stage == 3:
                out += [(self.view(unit, {a: low, b: self.prev[b], c: self.pos[c]}), self.right[b]),
                        (self.view(unit, {a: high, b: self.next[b], c: self.pos[c]}), self.left[b])]
            elif stage == 4:
                plane = {a: every, b: every, c: self.pos[c]}
                out += [(self.view(unit, plane), self.right[c]), (self.view(unit, plane), self.left[c])]
            else:
                slow, fast = (a, b) if 'zyx'.index(a) < 'zyx'.index(b) else (b, a)
                out += [(self.view(unit, {slow: low, fast: every, c: self.prev[c]}), self.right[c]),
                        (self.view(unit, {slow: high, fast: every, c: self.next[c]}), self.left[c])]
        return out

    def start(self, chunk, stage):
        for ref, dev in self.sends(chunk, stage):
            pltpu.make_async_remote_copy(
                src_ref=ref, dst_ref=ref, send_sem=self.send_sem.at[chunk, stage], recv_sem=self.recv_sem.at[chunk, stage],
                device_id={'wg': dev}, device_id_type=MESH).start()

    def wait(self, sem, chunk, stage):
        w = self.blocks
        size = (w.at[0:3, 0, 0, 0:2], w.at[0:3, 0, 0, 0], w.at[0:3, 0, 0:2], w.at[0:3, 0, 0], w.at[0:3, 0:2], w.at[0:3, 0])[stage]
        pltpu.make_async_copy(size, size, sem.at[chunk, stage]).wait()

    def step(self, chunk, stage):
        if stage > 0:
            self.wait(self.recv_sem, chunk, stage - 1)
        if stage < STAGES:
            self.start(chunk, stage)

    def poll(self, piece, layer, index):
        for at_layer, at_index, due in SCHEDULE.get(piece, ()):
            @pl.when((layer == at_layer) & (index == at_index))
            def _():
                for chunk, stage in due:
                    self.step(chunk, stage)


def normalize(values, scale, shift):
    mean = jnp.mean(values, axis=1, keepdims=True)
    centered = values - mean
    variance = jnp.mean(centered * centered, axis=1, keepdims=True)
    return (centered * lax.rsqrt(variance + LN_EPS) * scale + shift).astype(jnp.bfloat16)


def rows(r, size=256):
    return pl.ds(pl.multiple_of(r * size, size), size)


def layers_kernel(x_hbm, mask_ref, slope_ref, ln1s_ref, ln1b_ref, ln2s_ref, ln2b_ref, bqkv_ref, bout_ref, bup_ref, bdown_ref,
                  wout_ref, wqkv_hbm, wup_hbm, wdown_hbm, out_hbm, cache_hbm,
                  blocks, x, a, qkv, ctx, act, acc, part, other, bias_cols, limits, bias_rows,
                  send_sem, recv_sem, part_send, part_recv, own_sem, x_sem, cache_sem, out_sem):
    f32, bf16 = jnp.float32, jnp.bfloat16
    torus = Torus(blocks, send_sem, recv_sem)
    partner = {'tp': 1 - lax.axis_index('tp')}
    mine = (torus.pos['z'], torus.pos['y'], torus.pos['x'])
    own = []
    for layer in range(2):
        for first, weights, count in ((0, wqkv_hbm, 6), (8, wup_hbm, 8), (16, wdown_hbm, 8)):
            own += [pltpu.make_async_copy(weights.at[layer, :, j * 256:(j + 1) * 256],
                                          blocks.at[(layer * UNITS + first + j,) + mine], own_sem) for j in range(count)]
    for copy in own:
        copy.start()
    x_in = pltpu.make_async_copy(x_hbm, x, x_sem)
    x_in.start()
    for layer in range(2):
        flat = jnp.concatenate([wout_ref[layer, head] for head in range(8)], axis=1)
        for j in range(2):
            blocks[(layer * UNITS + 6 + j,) + mine] = flat[:, j * 256:(j + 1) * 256]
    torus.barrier()
    whole = blocks.at[0:44, 0, 0, 0]
    pltpu.make_async_copy(whole, whole, own_sem).wait()
    zero = jnp.int32(0)
    torus.poll('head', zero, zero)

    def row_of(ref, layer):
        both = ref[...].astype(f32)
        return jnp.where(layer == 0, both[0:1], both[1:2])

    def weight(unit):
        return blocks[unit].reshape(1024, 256)

    real = jnp.sum(mask_ref[...].astype(f32), axis=1, keepdims=True)
    key = lax.broadcasted_iota(jnp.int32, (1024, 128), 0).astype(f32)
    lane = lax.broadcasted_iota(jnp.int32, (1024, 128), 1)
    place = key - (1024.0 - real)
    slope = jnp.where(lax.axis_index('tp') == 0, slope_ref[0:1], slope_ref[1:2])
    key_bias = jnp.where(place >= 0.0, place * slope, -1e30)
    first = key_bias.astype(bf16)
    rest = key_bias - first.astype(f32)
    second = rest.astype(bf16)
    third = (rest - second.astype(f32)).astype(bf16)
    which = lax.rem(lane, 3)
    split = jnp.where(which == 0, first.astype(f32), jnp.where(which == 1, second.astype(f32), third.astype(f32)))
    bias_cols[...] = jnp.where(lane < 24, split, 0.0).astype(bf16)
    row = lax.broadcasted_iota(jnp.int32, (256, 256), 0)
    col = lax.broadcasted_iota(jnp.int32, (256, 256), 1)
    limits[0] = jnp.where(col <= row, 3e38, -1e30)
    limits[1] = jnp.where(col == row, -1e29, -3e38)

    for layer in range(2):
        for kind in range(3):
            heads = bqkv_ref[layer, kind].astype(f32)
            for j in range(2):
                bias_rows[layer * 6 + kind * 2 + j] = jnp.concatenate([heads[h:h + 1] for h in range(4 * j, 4 * j + 4)], axis=1)

    x_in.wait()

    def first_norm(r, carry):
        torus.poll('norm', zero, r)
        a[rows(r)] = normalize(x[rows(r)].astype(f32), ln1s_ref[0:1].astype(f32), ln1b_ref[0:1].astype(f32))
        return carry

    lax.fori_loop(0, 4, first_norm, 0)

    def exchange(layer, kind, r):
        view = lambda ref: ref.at[kind, rows(r)]
        return pltpu.make_async_remote_copy(
            src_ref=view(part), dst_ref=view(other), send_sem=part_send.at[layer, kind, r], recv_sem=part_recv.at[layer, kind, r],
            device_id=partner, device_id_type=MESH)

    def residual(layer, kind, r, bias):
        exchange(layer, kind, r).wait_recv()
        branch = part[kind, rows(r)].astype(f32) + other[kind, rows(r)].astype(f32)
        total = (x[rows(r)].astype(f32) + branch + bias).astype(bf16)
        x[rows(r)] = total
        return total.astype(f32)

    def attention(pair, carry):
        unit, lanes = lax.div(pair, 2), pl.ds(pl.multiple_of(lax.rem(pair, 2) * 128, 128), 128)
        lane = lax.broadcasted_iota(jnp.int32, (256, 128), 1)
        for r in range(4):
            n = (r + 1) * 256
            q = qkv[unit, r * 256:n, lanes]
            k = jnp.concatenate([qkv[2 + unit, 0:n, lanes], bias_cols[0:n]], axis=1)
            v = jnp.concatenate([qkv[4 + unit, 0:n, lanes], jnp.ones((n, 128), bf16)], axis=1)
            outs = []
            for half in range(2):
                mine = (lane < 64) if half == 0 else (lane >= 64)
                head = 2 * pair + half
                pick = ((lane >= 3 * head) & (lane < 3 * head + 3)).astype(bf16)
                query = jnp.concatenate([jnp.where(mine, q, jnp.zeros_like(q)), pick], axis=1)
                scores = lax.dot_general(query, k, NT, preferred_element_type=f32)
                last = jnp.maximum(jnp.minimum(scores[:, r * 256:], limits[0]), limits[1])
                scores = jnp.concatenate([scores[:, :r * 256], last], axis=1) if r else last
                probs = jnp.exp(scores - jnp.max(scores, axis=1, keepdims=True)).astype(bf16)
                out = jnp.dot(probs, v, preferred_element_type=f32)
                outs.append(out[:, :128] / out[:, 128:])
            ctx[unit, r * 256:n, lanes] = jnp.where(lane < 64, outs[0], outs[1]).astype(bf16)
        return carry

    def layer_body(layer, carry):
        base = layer * UNITS

        def qkv_unit(j, carry):
            torus.poll('qkv', layer, j)
            scale = jnp.where(j < 2, 0.125, 1.0)
            out = jnp.dot(a[...], weight(base + j), preferred_element_type=f32) + bias_rows[layer * 6 + j]
            qkv[j] = (out * scale).astype(bf16)
            return carry

        lax.fori_loop(0, 6, qkv_unit, 0)
        cache = pltpu.make_async_copy(qkv.at[2:6], cache_hbm.at[layer], cache_sem)
        cache.start()

        def attend_pair(pair, carry):
            torus.poll('attn', layer, pair)
            return attention(pair, carry)

        lax.fori_loop(0, 4, attend_pair, 0)

        def send_after(kind, r):
            @pl.when(r > 0)
            def _():
                exchange(layer, kind, r - 1).start()

        def project(r, carry):
            torus.poll('proj', layer, r)
            c = jnp.concatenate([ctx[0, rows(r)], ctx[1, rows(r)]], axis=1)
            w = jnp.concatenate([weight(base + 6), weight(base + 7)], axis=1)
            part[0, rows(r)] = lax.dot_general(c, w, NT, preferred_element_type=f32).astype(bf16)
            send_after(0, r)
            return carry

        lax.fori_loop(0, 4, project, 0)
        exchange(layer, 0, 3).start()

        def second_norm(r, carry):
            torus.poll('mid', layer, r)
            total = residual(layer, 0, r, row_of(bout_ref, layer))
            a[rows(r)] = normalize(total, row_of(ln2s_ref, layer), row_of(ln2b_ref, layer))
            return carry

        lax.fori_loop(0, 4, second_norm, 0)

        def up_unit(j, carry):
            torus.poll('up', layer, j)
            cols = pl.ds(pl.multiple_of(j * 256, 256), 256)
            both = bup_ref[:, cols].astype(f32)
            bias = jnp.where(layer == 0, both[0:1], both[1:2])
            out = jnp.dot(a[...], weight(base + 8 + j), preferred_element_type=f32) + bias
            act[j] = jax.nn.gelu(out, approximate=True).astype(bf16)
            return carry

        lax.fori_loop(0, 8, up_unit, 0)

        def down_product(r, units):
            h = jnp.concatenate([act[j, rows(r)] for j in units], axis=1)
            w = jnp.concatenate([weight(base + 16 + j) for j in units], axis=1)
            return lax.dot_general(h, w, NT, preferred_element_type=f32)

        def down_first(r, carry):
            torus.poll('d0', layer, r)
            acc[rows(r)] = down_product(r, (0, 1))
            return carry

        def down_next(r, carry):
            torus.poll('d1', layer, r)
            acc[rows(r)] += down_product(r, (2, 3, 4))
            return carry

        def down_last(r, carry):
            torus.poll('d2', layer, r)
            part[1, rows(r)] = (acc[rows(r)] + down_product(r, (5, 6, 7))).astype(bf16)
            send_after(1, r)
            return carry

        lax.fori_loop(0, 4, down_first, 0)
        lax.fori_loop(0, 4, down_next, 0)
        lax.fori_loop(0, 4, down_last, 0)
        cache.wait()
        exchange(layer, 1, 3).start()

        def finish(r, carry):
            torus.poll('fin', layer, r)
            total = residual(layer, 1, r, row_of(bdown_ref, layer))

            @pl.when(layer == 0)
            def _():
                a[rows(r)] = normalize(total, ln1s_ref[1:2].astype(f32), ln1b_ref[1:2].astype(f32))
            return carry

        lax.fori_loop(0, 4, finish, 0)

        def sent(r, carry):
            exchange(layer, 0, r).wait_send()
            exchange(layer, 1, r).wait_send()
            return carry

        lax.fori_loop(0, 4, sent, 0)
        return carry

    lax.fori_loop(0, 2, layer_body, 0)
    out = pltpu.make_async_copy(x, out_hbm, out_sem)
    out.start()

    def drain(chunk, carry):
        for stage in range(STAGES):
            torus.wait(send_sem, chunk, stage)
        return carry

    lax.fori_loop(0, CHUNKS, drain, 0)
    out.wait()


def run_layers(*operands):
    vmem, hbm = pl.BlockSpec(memory_space=pltpu.VMEM), pl.BlockSpec(memory_space=pl.ANY)
    bf16, dma = jnp.bfloat16, pltpu.SemaphoreType.DMA
    return pl.pallas_call(
        layers_kernel,
        out_shape=(jax.ShapeDtypeStruct((1024, 1024), bf16), jax.ShapeDtypeStruct((2, 4, 1024, 256), bf16)),
        in_specs=[hbm] + [vmem] * 11 + [hbm] * 3,
        out_specs=(hbm, hbm),
        scratch_shapes=[
            pltpu.VMEM((2 * UNITS, 4, 4, 4, 16, 256), bf16),
            pltpu.VMEM((1024, 1024), bf16),
            pltpu.VMEM((1024, 1024), bf16),
            pltpu.VMEM((6, 1024, 256), bf16),
            pltpu.VMEM((2, 1024, 256), bf16),
            pltpu.VMEM((8, 1024, 256), bf16),
            pltpu.VMEM((1024, 1024), jnp.float32),
            pltpu.VMEM((2, 1024, 1024), bf16),
            pltpu.VMEM((2, 1024, 1024), bf16),
            pltpu.VMEM((1024, 128), bf16),
            pltpu.VMEM((2, 256, 256), jnp.float32),
            pltpu.VMEM((12, 1, 256), jnp.float32),
            dma((CHUNKS, STAGES)),
            dma((CHUNKS, STAGES)),
            dma((2, 2, 4)),
            dma((2, 2, 4)),
            dma,
            dma,
            dma,
            dma,
        ],
        compiler_params=pltpu.CompilerParams(collective_id=0, has_side_effects=True, vmem_limit_bytes=67043328),
        name='two_layers',
    )(*operands)


def finish_kernel(x_ref, key_ref, value_ref, out_ref, key_out, value_out):
    out_ref[...] = x_ref[...]
    key_out[0] = key_ref[0, 0].T
    value_out[0] = value_ref[0, 0].T


def finish_outputs(x, cache):
    bf16 = jnp.bfloat16
    across = pl.BlockSpec((1, 128, 1024), lambda i: (i // 4, i % 4, 0))
    return pl.pallas_call(
        finish_kernel,
        grid=(8,),
        out_shape=(jax.ShapeDtypeStruct(x.shape, bf16),) + (jax.ShapeDtypeStruct((2, 512, 1024), bf16),) * 2,
        in_specs=[pl.BlockSpec((128, 1024), lambda i: (i, 0)),
                  pl.BlockSpec((1, 1, 1024, 128), lambda i: (i // 4, (i % 4) // 2, 0, i % 2)),
                  pl.BlockSpec((1, 1, 1024, 128), lambda i: (i // 4, 2 + (i % 4) // 2, 0, i % 2))],
        out_specs=(pl.BlockSpec((128, 1024), lambda i: (i, 0)), across, across),
        name='finish_outputs',
    )(x, cache, cache)


def solution(mesh):
    tp_size = mesh.shape['tp']
    batch_axes = ('dp', 'wg')

    def device_fn(hidden, attn_mask, ln1_scale, ln1_bias, w_qkv, b_qkv, w_out, b_out,
                  ln2_scale, ln2_bias, w_up, b_up, w_down, b_down):
        n_layers, _, local_heads, _, head_dim = w_qkv.shape
        slopes = np.zeros((tp_size, 128), np.float32)
        slopes[:, :3 * local_heads] = np.repeat(alibi_slopes(local_heads * tp_size).reshape(tp_size, local_heads), 3, axis=1)
        out, cache = run_layers(
            hidden.reshape(hidden.shape[1:]), attn_mask, slopes, ln1_scale, ln1_bias, ln2_scale, ln2_bias,
            b_qkv.transpose(0, 2, 1, 3), b_out, b_up, b_down, w_out.transpose(0, 1, 3, 2),
            w_qkv.transpose(0, 1, 3, 2, 4).reshape(n_layers, 16, -1), w_up, w_down.transpose(0, 2, 1))
        out, keys, values = finish_outputs(out, cache)
        caches = [c.reshape(n_layers, 1, local_heads, head_dim, 1024).transpose(0, 1, 4, 2, 3) for c in (keys, values)]
        return out.reshape(hidden.shape), *caches

    replicated = P(None, None)
    in_specs = (P(batch_axes, None, None), P(batch_axes, None), replicated, replicated,
                P(None, 'wg', 'tp', None, None), P(None, 'tp', None, None), P(None, 'tp', None, 'wg'), replicated,
                replicated, replicated, P(None, 'wg', 'tp'), P(None, 'tp'), P(None, 'tp', 'wg'), replicated)
    cache_spec = P(None, batch_axes, None, 'tp', None)
    out_specs = (P(batch_axes, None, None), cache_spec, cache_spec)
    return jax.shard_map(device_fn, mesh=mesh, in_specs=in_specs, out_specs=out_specs, check_vma=False)
```

```python
import math
import jax
import jax.numpy as jnp
import numpy as np
from jax import lax
from jax.experimental import pallas as pl
from jax.experimental.pallas import tpu as pltpu
from jax.sharding import PartitionSpec as P

LN_EPS = 1e-5
GELU_A = math.sqrt(2.0 / math.pi)
GELU_B = 0.044715 * GELU_A
MESH = pl.DeviceIdType.MESH
UNITS = 24
HALVES = 4
CHUNKS = 18
DIRECT = (0,)
STAGES = 6
SCHEDULE = {
    'head': ((0, 0, ((0, 0), (1, 0), (2, 0), (3, 0), (4, 0), (5, 0), (6, 0), (7, 0), (8, 0), (9, 0), (10, 0), (11, 0), (12, 0), (13, 0), (14, 0), (15, 0), (16, 0), (17, 0))),),
    'qkv': ((0, 0, ((0, 1), (0, 2), (0, 3), (9, 1), (1, 1), (2, 1), (3, 1), (4, 1), (5, 1), (6, 1), (7, 1), (8, 1), (10, 1), (11, 1), (12, 1), (13, 1), (14, 1), (15, 1), (16, 1), (9, 2), (1, 2), (2, 2), (7, 2), (0, 4), (9, 3), (3, 2), (4, 2), (2, 3), (7, 3), (1, 3), (5, 2), (0, 5), (6, 2), (3, 3), (4, 3), (8, 2), (7, 4), (0, 6), (1, 4))), (0, 1, ((1, 5), (2, 5), (4, 4), (1, 6), (5, 4))), (0, 2, ((2, 6), (4, 5))), (0, 3, ((3, 6),)), (1, 0, ((10, 6), (11, 5))), (1, 2, ((11, 6), (13, 5)))),
    'attn': ((0, 0, ((2, 4), (5, 3), (6, 3), (3, 4))), (0, 1, ((3, 5), (6, 4))), (0, 2, ((7, 5), (8, 3), (9, 4))), (0, 3, ((5, 5), (10, 2), (6, 5))), (1, 0, ((14, 4),)), (1, 1, ((12, 5), (15, 4))), (1, 2, ((16, 4),)), (1, 3, ((14, 5), (17, 3)))),
    'proj': ((0, 0, ((4, 6),)), (0, 2, ((8, 4),)), (1, 0, ((12, 6), (15, 5)))),
    'mid': ((0, 1, ((9, 5),)), (0, 3, ((11, 2),)), (1, 1, ((16, 5),))),
    'up': ((0, 0, ((10, 3), (12, 2))), (0, 1, ((5, 6), (13, 2))), (0, 2, ((14, 2), (15, 2))), (0, 3, ((16, 2),)), (0, 4, ((6, 6), (8, 5))), (0, 5, ((17, 1),)), (0, 6, ((11, 3),)), (0, 7, ((7, 6), (10, 4))), (1, 0, ((17, 4),)), (1, 1, ((13, 6),)), (1, 4, ((14, 6),)), (1, 7, ((15, 6),))),
    'd0': ((0, 2, ((12, 3), (13, 3))), (0, 3, ((14, 3),)), (1, 0, ((17, 5),))),
    'd1': ((0, 0, ((8, 6), (15, 3), (16, 3))), (0, 2, ((11, 4),)), (1, 0, ((16, 6),))),
    'd2': ((0, 0, ((9, 6), (17, 2))), (0, 2, ((10, 5),)), (0, 3, ((12, 4),)), (1, 0, ((17, 6),))),
    'fin': ((0, 2, ((13, 4),)),),
}
NT = (((1,), (1,)), ((), ()))
ORDERS = (('x', 'y', 'z'), ('y', 'z', 'x'), ('z', 'x', 'y'))


def alibi_slopes(n_heads):
    closest = 2 ** int(math.floor(math.log2(n_heads)))
    slope_base = 2.0 ** (-8.0 / closest)
    slope_list = [slope_base ** (i + 1) for i in range(closest)]
    extra_base = 2.0 ** (-4.0 / closest)
    slope_list = slope_list + [extra_base ** (2 * i + 1) for i in range(n_heads - closest)]
    return np.array(slope_list, dtype=np.float32)


class Torus:
    def __init__(self, blocks, send_sem, recv_sem):
        self.blocks, self.send_sem, self.recv_sem = blocks, send_sem, recv_sem
        me = lax.axis_index('wg')
        self.pos = {'z': lax.div(me, 16), 'y': lax.rem(lax.div(me, 4), 4), 'x': lax.rem(me, 4)}
        self.next = {ax: lax.rem(p + 1, 4) for ax, p in self.pos.items()}
        self.prev = {ax: lax.rem(p + 3, 4) for ax, p in self.pos.items()}
        self.right = {ax: self.device({**self.pos, ax: self.next[ax]}) for ax in 'zyx'}
        self.across = {ax: self.device({**self.pos, ax: lax.rem(self.pos[ax] + 2, 4)}) for ax in 'zyx'}
        self.left = {ax: self.device({**self.pos, ax: self.prev[ax]}) for ax in 'zyx'}

    @staticmethod
    def device(pos):
        return pos['z'] * 16 + pos['y'] * 4 + pos['x']

    def view(self, unit, where, cols=slice(0, 256)):
        return self.blocks.at[unit, where['z'], where['y'], where['x'], :, cols]

    def barrier(self):
        sem = pltpu.get_barrier_semaphore()
        for ax in 'zyx':
            for dev in (self.left[ax], self.right[ax], self.across[ax]):
                pl.semaphore_signal(sem, inc=1, device_id={'wg': dev}, device_id_type=MESH)
        pl.semaphore_signal(sem, inc=1, device_id={'tp': 1 - lax.axis_index('tp')}, device_id_type=MESH)
        pl.semaphore_wait(sem, 10)

    def part(self, chunk):
        if chunk < HALVES:
            return 3 * (chunk // 2), (chunk % 2) * 128, 128
        return 3 * (chunk - HALVES // 2), 0, 256

    def sends(self, chunk, stage):
        every, low, high = slice(None), slice(0, 2), slice(2, 4)
        first, start, width = self.part(chunk)
        cols = slice(start, start + width)
        out = []
        for color, (a, b, c) in enumerate(ORDERS):
            unit = first + color
            if stage in (0, 2, 4):
                axis = (a, b, c)[stage // 2]
                held = {**self.pos, **{ax: every for ax in (a, b)[:stage // 2]}}
                ref = self.view(unit, held, cols)
                out += [(ref, self.right[axis]), (ref, self.left[axis])]
                if chunk in DIRECT and stage < 4:
                    out.append((ref, self.across[axis]))
            elif stage == 1:
                ahead, back = {**self.pos, a: self.prev[a]}, {**self.pos, a: self.next[a]}
                if width == 256:
                    out += [(self.view(unit, ahead, slice(0, 128)), self.right[a]), (self.view(unit, back, slice(128, 256)), self.left[a])]
                elif chunk % 2 == 0:
                    out.append((self.view(unit, ahead, cols), self.right[a]))
                else:
                    out.append((self.view(unit, back, cols), self.left[a]))
            elif stage == 3:
                out += [(self.view(unit, {a: low, b: self.prev[b], c: self.pos[c]}, cols), self.right[b]),
                        (self.view(unit, {a: high, b: self.next[b], c: self.pos[c]}, cols), self.left[b])]
            else:
                slow, fast = (a, b) if 'zyx'.index(a) < 'zyx'.index(b) else (b, a)
                out += [(self.view(unit, {slow: low, fast: every, c: self.prev[c]}, cols), self.right[c]),
                        (self.view(unit, {slow: high, fast: every, c: self.next[c]}, cols), self.left[c])]
        return out

    def start(self, chunk, stage):
        for ref, dev in self.sends(chunk, stage):
            pltpu.make_async_remote_copy(
                src_ref=ref, dst_ref=ref, send_sem=self.send_sem.at[chunk, stage], recv_sem=self.recv_sem.at[chunk, stage],
                device_id={'wg': dev}, device_id_type=MESH).start()

    def wait(self, sem, chunk, stage):
        every, three = slice(None), slice(0, 3)
        peers = three if chunk in DIRECT else slice(0, 2)
        where = ((0, 0, peers), (0, 0, 0), (0, peers, every), (0, 0, every), (slice(0, 2), every, every), (0, every, every))[stage]
        size = self.blocks.at[(three,) + where + (every, slice(0, self.part(chunk)[2]))]
        pltpu.make_async_copy(size, size, sem.at[chunk, stage]).wait()

    def used(self, chunk, stage):
        return stage < STAGES and not (chunk in DIRECT and stage in (1, 3))

    def step(self, chunk, stage):
        before = [n for n in range(stage) if self.used(chunk, n)]
        if stage < STAGES and not self.used(chunk, stage):
            return
        if before:
            self.wait(self.recv_sem, chunk, before[-1])
        if stage < STAGES:
            self.start(chunk, stage)

    def poll(self, piece, layer, index):
        for at_layer, at_index, due in SCHEDULE.get(piece, ()):
            @pl.when((layer == at_layer) & (index == at_index))
            def _():
                for chunk, stage in due:
                    self.step(chunk, stage)


def normalize(values, scale, shift):
    mean = jnp.mean(values, axis=1, keepdims=True)
    centered = values - mean
    variance = jnp.mean(centered * centered, axis=1, keepdims=True)
    return (centered * lax.rsqrt(variance + LN_EPS) * scale + shift).astype(jnp.bfloat16)


def gelu(h):
    half = 0.5 * h
    return half + half * jnp.tanh(h * (GELU_A + GELU_B * (h * h)))


def rows(r, size=256):
    return pl.ds(pl.multiple_of(r * size, size), size)


def layers_kernel(x_hbm, mask_ref, slope_ref, ln1s_ref, ln1b_ref, ln2s_ref, ln2b_ref, bqkv_ref, bout_ref, bup_ref, bdown_ref,
                  wout_ref, wqkv_hbm, wup_hbm, wdown_hbm, out_hbm, key_hbm, value_hbm,
                  blocks, x, a, qkv, ctx, act, acc, part, other, bias_cols, limits, bias_rows, keys, values,
                  send_sem, recv_sem, part_send, part_recv, own_sem, x_sem, key_sem, value_sem, out_sem):
    f32, bf16 = jnp.float32, jnp.bfloat16
    torus = Torus(blocks, send_sem, recv_sem)
    partner = {'tp': 1 - lax.axis_index('tp')}
    mine = (torus.pos['z'], torus.pos['y'], torus.pos['x'])
    own = []
    for layer in range(2):
        for first, weights, count in ((0, wqkv_hbm, 6), (8, wup_hbm, 8), (16, wdown_hbm, 8)):
            for j in range(count):
                at = (j % 3) * 512 + (j // 3) * 256 if first == 0 else j * 256
                own.append(pltpu.make_async_copy(weights.at[layer, :, at:at + 256],
                                                 blocks.at[(layer * UNITS + first + j,) + mine], own_sem))
    for copy in own:
        copy.start()
    x_in = pltpu.make_async_copy(x_hbm, x, x_sem)
    x_in.start()
    for layer in range(2):
        flat = jnp.concatenate([wout_ref[layer, head] for head in range(8)], axis=1)
        for j in range(2):
            blocks[(layer * UNITS + 6 + j,) + mine] = flat[:, j * 256:(j + 1) * 256]
    torus.barrier()
    whole = blocks.at[0:44, 0, 0, 0]
    pltpu.make_async_copy(whole, whole, own_sem).wait()
    zero = jnp.int32(0)
    torus.poll('head', zero, zero)

    def row_of(ref, layer):
        both = ref[...].astype(f32)
        return jnp.where(layer == 0, both[0:1], both[1:2])

    def weight(unit):
        return blocks[unit].reshape(1024, 256)

    real = jnp.sum(mask_ref[...].astype(f32), axis=1, keepdims=True)
    key = lax.broadcasted_iota(jnp.int32, (1024, 128), 0).astype(f32)
    lane = lax.broadcasted_iota(jnp.int32, (1024, 128), 1)
    place = key - (1024.0 - real)
    slope = jnp.where(lax.axis_index('tp') == 0, slope_ref[0:1], slope_ref[1:2])
    key_bias = jnp.where(place >= 0.0, place * slope, -1e30)
    first = key_bias.astype(bf16)
    rest = key_bias - first.astype(f32)
    second = rest.astype(bf16)
    third = (rest - second.astype(f32)).astype(bf16)
    which = lax.rem(lane, 3)
    split = jnp.where(which == 0, first.astype(f32), jnp.where(which == 1, second.astype(f32), third.astype(f32)))
    bias_cols[...] = jnp.where(lane < 24, split, 0.0).astype(bf16)
    row = lax.broadcasted_iota(jnp.int32, (256, 256), 0)
    col = lax.broadcasted_iota(jnp.int32, (256, 256), 1)
    limits[0] = jnp.where(col <= row, 3e38, -1e30)
    limits[1] = jnp.where(col == row, -1e29, -3e38)

    for layer in range(2):
        for kind in range(3):
            heads = bqkv_ref[layer, kind].astype(f32)
            for j in range(2):
                bias_rows[layer * 6 + kind * 2 + j] = jnp.concatenate([heads[h:h + 1] for h in range(4 * j, 4 * j + 4)], axis=1)

    x_in.wait()

    def first_norm(r, carry):
        torus.poll('norm', zero, r)
        a[rows(r)] = normalize(x[rows(r)].astype(f32), ln1s_ref[0:1].astype(f32), ln1b_ref[0:1].astype(f32))
        return carry

    lax.fori_loop(0, 4, first_norm, 0)

    def exchange(layer, kind, r):
        view = lambda ref: ref.at[kind, rows(r)]
        return pltpu.make_async_remote_copy(
            src_ref=view(part), dst_ref=view(other), send_sem=part_send.at[layer, kind, r], recv_sem=part_recv.at[layer, kind, r],
            device_id=partner, device_id_type=MESH)

    def residual(layer, kind, r, bias):
        exchange(layer, kind, r).wait_recv()
        branch = part[kind, rows(r)].astype(f32) + other[kind, rows(r)].astype(f32)
        total = (x[rows(r)].astype(f32) + branch + bias).astype(bf16)
        x[rows(r)] = total
        return total.astype(f32)

    def attention(layer, pair, carry):
        unit, lanes = lax.div(pair, 2), pl.ds(pl.multiple_of(lax.rem(pair, 2) * 128, 128), 128)
        lane = lax.broadcasted_iota(jnp.int32, (256, 128), 1)
        for r in range(4):
            n = (r + 1) * 256
            q = qkv[unit, r * 256:n, lanes]
            k = jnp.concatenate([qkv[2 + unit, 0:n, lanes], bias_cols[0:n]], axis=1)
            v = jnp.concatenate([qkv[4 + unit, 0:n, lanes], jnp.ones((n, 128), bf16)], axis=1)
            queries, probs = [], []
            for half in range(2):
                mine = (lane < 64) if half == 0 else (lane >= 64)
                head = 2 * pair + half
                pick = ((lane >= 3 * head) & (lane < 3 * head + 3)).astype(bf16)
                queries.append(jnp.concatenate([jnp.where(mine, q, jnp.zeros_like(q)), pick], axis=1))
            both = lax.dot_general(jnp.concatenate(queries, axis=0), k, NT, preferred_element_type=f32)
            for half in range(2):
                scores = both[half * 256:(half + 1) * 256]
                last = jnp.maximum(jnp.minimum(scores[:, r * 256:], limits[0]), limits[1])
                scores = jnp.concatenate([scores[:, :r * 256], last], axis=1) if r else last
                probs.append(jnp.exp(scores - jnp.max(scores, axis=1, keepdims=True)).astype(bf16))
            out = jnp.dot(jnp.concatenate(probs, axis=0), v, preferred_element_type=f32)
            outs = [out[half * 256:(half + 1) * 256, :128] / out[half * 256:(half + 1) * 256, 128:] for half in range(2)]
            ctx[unit, r * 256:n, lanes] = jnp.where(lane < 64, outs[0], outs[1]).astype(bf16)
        return carry

    def leave(r):
        return pltpu.make_async_copy(x.at[rows(r)], out_hbm.at[rows(r)], out_sem.at[r])

    def layer_body(layer, carry):
        base = layer * UNITS

        def project_in(half, width, start):
            cols = pl.ds(start, width)
            w = jnp.concatenate([blocks[base + 3 * half + kind, :, :, :, :, cols].reshape(1024, width) for kind in range(3)], axis=1)
            out = jnp.dot(a[...], w, preferred_element_type=f32)
            for kind in range(3):
                slot = 2 * kind + half
                piece = out[:, kind * width:(kind + 1) * width] + bias_rows[layer * 6 + slot, :, cols]
                qkv[slot, :, cols] = (piece * 0.125 if kind == 0 else piece).astype(bf16)

        caches = (pltpu.make_async_copy(keys, key_hbm.at[layer], key_sem),
                  pltpu.make_async_copy(values, value_hbm.at[layer], value_sem))

        def attend_pair(pair, carry):
            torus.poll('qkv', layer, pair)
            half, second = lax.div(pair, 2), lax.rem(pair, 2)

            @pl.when(layer == 0)
            def _():
                project_in(half, 128, pl.multiple_of(second * 128, 128))

            @pl.when((layer == 1) & (second == 0))
            def _():
                project_in(half, 256, 0)

            torus.poll('attn', layer, pair)
            attention(layer, pair, carry)

            @pl.when(second == 1)
            def _():
                keys[rows(half)] = qkv[2 + half].T
                values[rows(half)] = qkv[4 + half].T
            return carry

        lax.fori_loop(0, 4, attend_pair, 0)
        for cache in caches:
            cache.start()

        def send_after(kind, r):
            @pl.when(r > 0)
            def _():
                exchange(layer, kind, r - 1).start()

        def project(r, carry):
            torus.poll('proj', layer, r)
            c = jnp.concatenate([ctx[0, rows(r)], ctx[1, rows(r)]], axis=1)
            w = jnp.concatenate([weight(base + 6), weight(base + 7)], axis=1)
            part[0, rows(r)] = lax.dot_general(c, w, NT, preferred_element_type=f32).astype(bf16)
            send_after(0, r)
            return carry

        lax.fori_loop(0, 4, project, 0)
        exchange(layer, 0, 3).start()

        def second_norm(r, carry):
            torus.poll('mid', layer, r)
            total = residual(layer, 0, r, row_of(bout_ref, layer))
            a[rows(r)] = normalize(total, row_of(ln2s_ref, layer), row_of(ln2b_ref, layer))
            return carry

        lax.fori_loop(0, 4, second_norm, 0)

        def up_unit(j, carry):
            torus.poll('up', layer, j)
            cols = pl.ds(pl.multiple_of(j * 256, 256), 256)
            both = bup_ref[:, cols].astype(f32)
            bias = jnp.where(layer == 0, both[0:1], both[1:2])
            out = jnp.dot(a[...], weight(base + 8 + j), preferred_element_type=f32) + bias
            act[j] = gelu(out).astype(bf16)
            return carry

        lax.fori_loop(0, 8, up_unit, 0)

        def down_product(r, units):
            h = jnp.concatenate([act[j, rows(r)] for j in units], axis=1)
            w = jnp.concatenate([weight(base + 16 + j) for j in units], axis=1)
            return lax.dot_general(h, w, NT, preferred_element_type=f32)

        def down_first(r, carry):
            torus.poll('d0', layer, r)
            acc[rows(r)] = down_product(r, (0, 1))
            return carry

        def down_next(r, carry):
            torus.poll('d1', layer, r)
            acc[rows(r)] += down_product(r, (2, 3, 4))
            return carry

        def down_last(r, carry):
            torus.poll('d2', layer, r)
            part[1, rows(r)] = (acc[rows(r)] + down_product(r, (5, 6, 7))).astype(bf16)
            send_after(1, r)
            return carry

        lax.fori_loop(0, 4, down_first, 0)
        lax.fori_loop(0, 4, down_next, 0)
        lax.fori_loop(0, 4, down_last, 0)
        for cache in caches:
            cache.wait()
        exchange(layer, 1, 3).start()

        def finish(r, carry):
            torus.poll('fin', layer, r)
            total = residual(layer, 1, r, row_of(bdown_ref, layer))

            @pl.when(layer == 0)
            def _():
                a[rows(r)] = normalize(total, ln1s_ref[1:2].astype(f32), ln1b_ref[1:2].astype(f32))

            @pl.when((layer == 1) & (r > 0))
            def _():
                leave(r - 1).start()
            return carry

        lax.fori_loop(0, 4, finish, 0)

        def sent(r, carry):
            exchange(layer, 0, r).wait_send()
            exchange(layer, 1, r).wait_send()
            return carry

        lax.fori_loop(0, 4, sent, 0)
        return carry

    lax.fori_loop(0, 2, layer_body, 0)
    leave(3).start()
    for chunk in range(CHUNKS):
        for stage in range(STAGES):
            if torus.used(chunk, stage):
                torus.wait(send_sem, chunk, stage)
    for r in range(4):
        leave(r).wait()


def run_layers(*operands):
    vmem, hbm = pl.BlockSpec(memory_space=pltpu.VMEM), pl.BlockSpec(memory_space=pl.ANY)
    bf16, dma = jnp.bfloat16, pltpu.SemaphoreType.DMA
    return pl.pallas_call(
        layers_kernel,
        out_shape=(jax.ShapeDtypeStruct((1024, 1024), bf16),) + (jax.ShapeDtypeStruct((2, 512, 1024), bf16),) * 2,
        in_specs=[hbm] + [vmem] * 11 + [hbm] * 3,
        out_specs=(hbm,) * 3,
        scratch_shapes=[
            pltpu.VMEM((2 * UNITS, 4, 4, 4, 16, 256), bf16),
            pltpu.VMEM((1024, 1024), bf16),
            pltpu.VMEM((1024, 1024), bf16),
            pltpu.VMEM((6, 1024, 256), bf16),
            pltpu.VMEM((2, 1024, 256), bf16),
            pltpu.VMEM((8, 1024, 256), bf16),
            pltpu.VMEM((1024, 1024), jnp.float32),
            pltpu.VMEM((2, 1024, 1024), bf16),
            pltpu.VMEM((2, 1024, 1024), bf16),
            pltpu.VMEM((1024, 128), bf16),
            pltpu.VMEM((2, 256, 256), jnp.float32),
            pltpu.VMEM((12, 1, 256), jnp.float32),
            pltpu.VMEM((512, 1024), bf16),
            pltpu.VMEM((512, 1024), bf16),
            dma((CHUNKS, STAGES)),
            dma((CHUNKS, STAGES)),
            dma((2, 2, 4)),
            dma((2, 2, 4)),
            dma,
            dma,
            dma,
            dma,
            dma((4,)),
        ],
        compiler_params=pltpu.CompilerParams(collective_id=0, has_side_effects=True, vmem_limit_bytes=58*2**20),
        name='two_layers',
    )(*operands)


PIECES = 4


def pass_kernel(*refs):
    sources, targets, (held, in_sem, out_sem) = refs[:3], refs[3:6], refs[6:]
    size = 1024 // PIECES
    views = [(k * PIECES + p, sources[k].at[p * size:(p + 1) * size], targets[k].at[p * size:(p + 1) * size])
             for p in range(PIECES) for k in range(3)]
    into = [pltpu.make_async_copy(src, held.at[n], in_sem.at[n]) for n, src, _ in views]
    out = [pltpu.make_async_copy(held.at[n], dst, out_sem.at[n]) for n, _, dst in views]
    for copy in into:
        copy.start()
    for first, second in zip(into, out):
        first.wait()
        second.start()
    for copy in out:
        copy.wait()


def pass_on(*arrays):
    shape = jax.ShapeDtypeStruct((1024, 1024), jnp.bfloat16)
    dma = pltpu.SemaphoreType.DMA
    return pl.pallas_call(
        pass_kernel,
        out_shape=(shape,) * 3,
        in_specs=[pl.BlockSpec(memory_space=pl.ANY)] * 3,
        out_specs=(pl.BlockSpec(memory_space=pl.ANY),) * 3,
        scratch_shapes=[pltpu.VMEM((3 * PIECES, 1024 // PIECES, 1024), jnp.bfloat16), dma((3 * PIECES,)), dma((3 * PIECES,))],
        name='pass_on',
    )(*arrays)


def solution(mesh):
    tp_size = mesh.shape['tp']
    batch_axes = ('dp', 'wg')

    def device_fn(hidden, attn_mask, ln1_scale, ln1_bias, w_qkv, b_qkv, w_out, b_out,
                  ln2_scale, ln2_bias, w_up, b_up, w_down, b_down):
        n_layers, _, local_heads, _, head_dim = w_qkv.shape
        slopes = np.zeros((tp_size, 128), np.float32)
        slopes[:, :3 * local_heads] = np.repeat(alibi_slopes(local_heads * tp_size).reshape(tp_size, local_heads), 3, axis=1)
        out, keys, values = run_layers(
            hidden.reshape(hidden.shape[1:]), attn_mask, slopes, ln1_scale, ln1_bias, ln2_scale, ln2_bias,
            b_qkv.transpose(0, 2, 1, 3), b_out, b_up, b_down, w_out.transpose(0, 1, 3, 2),
            w_qkv.transpose(0, 1, 3, 2, 4).reshape(n_layers, 16, -1), w_up, w_down.transpose(0, 2, 1))
        out, keys, values = pass_on(out, keys.reshape(1024, 1024), values.reshape(1024, 1024))
        caches = [c.reshape(n_layers, 1, local_heads, head_dim, 1024).transpose(0, 1, 4, 2, 3) for c in (keys, values)]
        return out.reshape(hidden.shape), *caches

    replicated = P(None, None)
    in_specs = (P(batch_axes, None, None), P(batch_axes, None), replicated, replicated,
                P(None, 'wg', 'tp', None, None), P(None, 'tp', None, None), P(None, 'tp', None, 'wg'), replicated,
                replicated, replicated, P(None, 'wg', 'tp'), P(None, 'tp'), P(None, 'tp', 'wg'), replicated)
    cache_spec = P(None, batch_axes, None, 'tp', None)
    out_specs = (P(batch_axes, None, None), cache_spec, cache_spec)
    return jax.shard_map(device_fn, mesh=mesh, in_specs=in_specs, out_specs=out_specs, check_vma=False)
```

```python
import math
import jax
import jax.numpy as jnp
import numpy as np
from jax import lax
from jax.experimental import pallas as pl
from jax.experimental.pallas import tpu as pltpu
from jax.sharding import PartitionSpec as P

LN_EPS = 1e-5
GELU_A = math.sqrt(2.0 / math.pi)
GELU_B = 0.044715 * GELU_A
MESH = pl.DeviceIdType.MESH
UNITS = 24
HALVES = 4
CHUNKS = 18
DIRECT = (0,)
STAGES = 6
SCHEDULE = {
    'head': ((0, 0, ((0, 0), (1, 0), (2, 0), (3, 0), (4, 0), (5, 0), (6, 0), (7, 0), (8, 0), (9, 0), (10, 0), (11, 0), (12, 0), (13, 0), (14, 0), (15, 0), (16, 0), (17, 0))),),
    'norm': ((0, 2, ((1, 1), (2, 1), (3, 1), (4, 1))), (0, 3, ((0, 1), (0, 2), (5, 1), (6, 1), (7, 1), (8, 1), (9, 1)))),
    'qkv': ((0, 0, ((0, 3), (1, 2), (2, 2), (3, 2), (4, 2), (5, 2), (0, 4), (1, 3), (2, 3), (3, 3), (4, 3), (5, 3), (0, 5), (1, 4), (2, 4), (3, 4), (5, 4), (0, 6))), (0, 1, ((2, 5), (4, 4), (5, 5), (3, 5), (1, 6))), (0, 2, ((2, 6), (4, 5), (9, 2))), (0, 3, ((3, 6), (7, 3), (8, 3))), (1, 0, ((12, 4), (10, 6))), (1, 2, ((12, 5), (13, 4), (11, 6), (14, 4)))),
    'attn': ((0, 0, ((1, 5),)), (0, 1, ((6, 2), (7, 2), (8, 2))), (0, 2, ((10, 1), (11, 1), (12, 1), (13, 1), (14, 1), (6, 3), (15, 1), (16, 1), (17, 1))), (0, 3, ((6, 4), (9, 3), (10, 2))), (1, 0, ((13, 3), (14, 3), (15, 3), (16, 3), (17, 3))), (1, 1, ((11, 5),)), (1, 3, ((15, 4),))),
    'proj': ((0, 0, ((4, 6), (7, 4))), (1, 0, ((12, 6), (13, 5)))),
    'mid': ((0, 0, ((8, 4),)), (1, 0, ((14, 5), (16, 4)))),
    'up': ((0, 0, ((6, 5),)), (0, 1, ((5, 6), (9, 4))), (0, 4, ((7, 5), (10, 3), (8, 5), (6, 6))), (0, 6, ((11, 2),)), (0, 7, ((12, 2), (9, 5), (7, 6))), (1, 0, ((15, 5),)), (1, 1, ((13, 6), (17, 4))), (1, 4, ((14, 6),)), (1, 5, ((16, 5),)), (1, 7, ((15, 6),))),
    'd1': ((0, 0, ((10, 4), (8, 6))), (0, 1, ((11, 3),)), (0, 2, ((12, 3), (13, 2))), (0, 3, ((14, 2),)), (1, 0, ((17, 5), (16, 6)))),
    'd2': ((0, 0, ((9, 6), (15, 2))), (0, 1, ((16, 2),)), (0, 2, ((17, 2),)), (0, 3, ((10, 5),)), (1, 0, ((17, 6),))),
    'fin': ((0, 0, ((11, 4),)),),
}
NT = (((1,), (1,)), ((), ()))
ORDERS = (('x', 'y', 'z'), ('y', 'z', 'x'), ('z', 'x', 'y'))


def alibi_slopes(n_heads):
    closest = 2 ** int(math.floor(math.log2(n_heads)))
    slope_base = 2.0 ** (-8.0 / closest)
    slope_list = [slope_base ** (i + 1) for i in range(closest)]
    extra_base = 2.0 ** (-4.0 / closest)
    slope_list = slope_list + [extra_base ** (2 * i + 1) for i in range(n_heads - closest)]
    return np.array(slope_list, dtype=np.float32)


class Torus:
    def __init__(self, blocks, send_sem, recv_sem):
        self.blocks, self.send_sem, self.recv_sem = blocks, send_sem, recv_sem
        me = lax.axis_index('wg')
        self.pos = {'z': lax.div(me, 16), 'y': lax.rem(lax.div(me, 4), 4), 'x': lax.rem(me, 4)}
        self.next = {ax: lax.rem(p + 1, 4) for ax, p in self.pos.items()}
        self.prev = {ax: lax.rem(p + 3, 4) for ax, p in self.pos.items()}
        self.right = {ax: self.device({**self.pos, ax: self.next[ax]}) for ax in 'zyx'}
        self.across = {ax: self.device({**self.pos, ax: lax.rem(self.pos[ax] + 2, 4)}) for ax in 'zyx'}
        self.left = {ax: self.device({**self.pos, ax: self.prev[ax]}) for ax in 'zyx'}

    @staticmethod
    def device(pos):
        return pos['z'] * 16 + pos['y'] * 4 + pos['x']

    def view(self, unit, where, cols=slice(0, 256)):
        return self.blocks.at[unit, where['z'], where['y'], where['x'], :, cols]

    def greet(self):
        sem = pltpu.get_barrier_semaphore()
        for ax in 'zyx':
            for dev in (self.left[ax], self.right[ax], self.across[ax]):
                pl.semaphore_signal(sem, inc=1, device_id={'wg': dev}, device_id_type=MESH)
        pl.semaphore_signal(sem, inc=1, device_id={'tp': 1 - lax.axis_index('tp')}, device_id_type=MESH)

    def meet(self):
        pl.semaphore_wait(pltpu.get_barrier_semaphore(), 10)

    def part(self, chunk):
        if chunk < HALVES:
            return 3 * (chunk // 2), (chunk % 2) * 128, 128
        return 3 * (chunk - HALVES // 2), 0, 256

    def sends(self, chunk, stage):
        every, low, high = slice(None), slice(0, 2), slice(2, 4)
        first, start, width = self.part(chunk)
        cols = slice(start, start + width)
        out = []
        for color, (a, b, c) in enumerate(ORDERS):
            unit = first + color
            if stage in (0, 2, 4):
                axis = (a, b, c)[stage // 2]
                held = {**self.pos, **{ax: every for ax in (a, b)[:stage // 2]}}
                ref = self.view(unit, held, cols)
                out += [(ref, self.right[axis]), (ref, self.left[axis])]
                if chunk in DIRECT and stage < 4:
                    out.append((ref, self.across[axis]))
            elif stage == 1:
                ahead, back = {**self.pos, a: self.prev[a]}, {**self.pos, a: self.next[a]}
                if width == 256:
                    out += [(self.view(unit, ahead, slice(0, 128)), self.right[a]), (self.view(unit, back, slice(128, 256)), self.left[a])]
                elif chunk % 2 == 0:
                    out.append((self.view(unit, ahead, cols), self.right[a]))
                else:
                    out.append((self.view(unit, back, cols), self.left[a]))
            elif stage == 3:
                out += [(self.view(unit, {a: low, b: self.prev[b], c: self.pos[c]}, cols), self.right[b]),
                        (self.view(unit, {a: high, b: self.next[b], c: self.pos[c]}, cols), self.left[b])]
            else:
                slow, fast = (a, b) if 'zyx'.index(a) < 'zyx'.index(b) else (b, a)
                out += [(self.view(unit, {slow: low, fast: every, c: self.prev[c]}, cols), self.right[c]),
                        (self.view(unit, {slow: high, fast: every, c: self.next[c]}, cols), self.left[c])]
        return out

    def start(self, chunk, stage):
        for ref, dev in self.sends(chunk, stage):
            pltpu.make_async_remote_copy(
                src_ref=ref, dst_ref=ref, send_sem=self.send_sem.at[chunk, stage], recv_sem=self.recv_sem.at[chunk, stage],
                device_id={'wg': dev}, device_id_type=MESH).start()

    def wait(self, sem, chunk, stage):
        every, three = slice(None), slice(0, 3)
        peers = three if chunk in DIRECT else slice(0, 2)
        where = ((0, 0, peers), (0, 0, 0), (0, peers, every), (0, 0, every), (slice(0, 2), every, every), (0, every, every))[stage]
        size = self.blocks.at[(three,) + where + (every, slice(0, self.part(chunk)[2]))]
        pltpu.make_async_copy(size, size, sem.at[chunk, stage]).wait()

    def used(self, chunk, stage):
        return stage < STAGES and not (chunk in DIRECT and stage in (1, 3))

    def step(self, chunk, stage):
        before = [n for n in range(stage) if self.used(chunk, n)]
        if stage < STAGES and not self.used(chunk, stage):
            return
        if before:
            self.wait(self.recv_sem, chunk, before[-1])
        if stage < STAGES:
            self.start(chunk, stage)

    def poll(self, piece, layer, index):
        for at_layer, at_index, due in SCHEDULE.get(piece, ()):
            @pl.when((layer == at_layer) & (index == at_index))
            def _():
                for chunk, stage in due:
                    self.step(chunk, stage)


def normalize(values, scale, shift):
    mean = jnp.mean(values, axis=1, keepdims=True)
    centered = values - mean
    variance = jnp.mean(centered * centered, axis=1, keepdims=True)
    return (centered * lax.rsqrt(variance + LN_EPS) * scale + shift).astype(jnp.bfloat16)


def gelu(h):
    half = 0.5 * h
    return half + half * jnp.tanh(h * (GELU_A + GELU_B * (h * h)))


def rows(r, size=256):
    return pl.ds(pl.multiple_of(r * size, size), size)


def layers_kernel(x_hbm, mask_ref, slope_ref, ln1s_ref, ln1b_ref, ln2s_ref, ln2b_ref, bqkv_ref, bout_ref, bup_ref, bdown_ref,
                  wout_ref, wqkv_ref, wup_hbm, wdown_hbm, out_hbm, key_hbm, value_hbm,
                  blocks, x, a, qkv, ctx, act, acc, part, other, bias_cols, limits, bias_rows, keys, values,
                  send_sem, recv_sem, part_send, part_recv, own_sem, x_sem, key_sem, value_sem, out_sem):
    f32, bf16 = jnp.float32, jnp.bfloat16
    torus = Torus(blocks, send_sem, recv_sem)
    partner = {'tp': 1 - lax.axis_index('tp')}
    mine = (torus.pos['z'], torus.pos['y'], torus.pos['x'])
    own = []
    torus.greet()
    for layer in range(2):
        for first, weights in ((8, wup_hbm), (16, wdown_hbm)):
            own += [pltpu.make_async_copy(weights.at[layer, :, j * 256:(j + 1) * 256],
                                          blocks.at[(layer * UNITS + first + j,) + mine], own_sem) for j in range(8)]
    for copy in own:
        copy.start()
    x_in = pltpu.make_async_copy(x_hbm, x, x_sem)
    x_in.start()
    for layer in range(2):
        flat = jnp.concatenate([wout_ref[layer, head] for head in range(8)], axis=1)
        for j in range(2):
            blocks[(layer * UNITS + 6 + j,) + mine] = flat[:, j * 256:(j + 1) * 256]
    for layer in range(2):
        for half in range(2):
            for kind in range(3):
                heads = [wqkv_ref[layer, :, kind, h, :] for h in range(4 * half, 4 * half + 4)]
                blocks[(layer * UNITS + 3 * half + kind,) + mine] = jnp.concatenate(heads, axis=1)
    torus.meet()
    whole = blocks.at[0:32, 0, 0, 0]
    pltpu.make_async_copy(whole, whole, own_sem).wait()
    zero = jnp.int32(0)
    torus.poll('head', zero, zero)

    def row_of(ref, layer):
        both = ref[...].astype(f32)
        return jnp.where(layer == 0, both[0:1], both[1:2])

    def weight(unit):
        return blocks[unit].reshape(1024, 256)

    real = jnp.sum(mask_ref[...].astype(f32), axis=1, keepdims=True)
    key = lax.broadcasted_iota(jnp.int32, (1024, 128), 0).astype(f32)
    lane = lax.broadcasted_iota(jnp.int32, (1024, 128), 1)
    place = key - (1024.0 - real)
    slope = jnp.where(lax.axis_index('tp') == 0, slope_ref[0:1], slope_ref[1:2])
    key_bias = jnp.where(place >= 0.0, place * slope, -1e30)
    first = key_bias.astype(bf16)
    rest = key_bias - first.astype(f32)
    second = rest.astype(bf16)
    third = (rest - second.astype(f32)).astype(bf16)
    which = lax.rem(lane, 3)
    split = jnp.where(which == 0, first.astype(f32), jnp.where(which == 1, second.astype(f32), third.astype(f32)))
    bias_cols[...] = jnp.where(lane < 24, split, 0.0).astype(bf16)
    row = lax.broadcasted_iota(jnp.int32, (256, 256), 0)
    col = lax.broadcasted_iota(jnp.int32, (256, 256), 1)
    limits[0] = jnp.where(col <= row, 3e38, -1e30)
    limits[1] = jnp.where(col == row, -1e29, -3e38)

    for layer in range(2):
        for kind in range(3):
            heads = bqkv_ref[layer, kind].astype(f32)
            for j in range(2):
                bias_rows[layer * 6 + kind * 2 + j] = jnp.concatenate([heads[h:h + 1] for h in range(4 * j, 4 * j + 4)], axis=1)

    x_in.wait()

    def first_norm(r, carry):
        torus.poll('norm', zero, r)
        a[rows(r)] = normalize(x[rows(r)].astype(f32), ln1s_ref[0:1].astype(f32), ln1b_ref[0:1].astype(f32))
        return carry

    lax.fori_loop(0, 4, first_norm, 0)

    def exchange(layer, kind, r):
        view = lambda ref: ref.at[kind, rows(r)]
        return pltpu.make_async_remote_copy(
            src_ref=view(part), dst_ref=view(other), send_sem=part_send.at[layer, kind, r], recv_sem=part_recv.at[layer, kind, r],
            device_id=partner, device_id_type=MESH)

    def residual(layer, kind, r, bias):
        exchange(layer, kind, r).wait_recv()
        branch = part[kind, rows(r)].astype(f32) + other[kind, rows(r)].astype(f32)
        total = (x[rows(r)].astype(f32) + branch + bias).astype(bf16)
        x[rows(r)] = total
        return total.astype(f32)

    def attention(layer, pair, carry):
        unit, lanes = lax.div(pair, 2), pl.ds(pl.multiple_of(lax.rem(pair, 2) * 128, 128), 128)
        lane = lax.broadcasted_iota(jnp.int32, (256, 128), 1)
        for r in range(4):
            n = (r + 1) * 256
            q = qkv[unit, r * 256:n, lanes]
            k = jnp.concatenate([qkv[2 + unit, 0:n, lanes], bias_cols[0:n]], axis=1)
            v = jnp.concatenate([qkv[4 + unit, 0:n, lanes], jnp.ones((n, 128), bf16)], axis=1)
            queries, probs = [], []
            for half in range(2):
                mine = (lane < 64) if half == 0 else (lane >= 64)
                head = 2 * pair + half
                pick = ((lane >= 3 * head) & (lane < 3 * head + 3)).astype(bf16)
                queries.append(jnp.concatenate([jnp.where(mine, q, jnp.zeros_like(q)), pick], axis=1))
            both = lax.dot_general(jnp.concatenate(queries, axis=0), k, NT, preferred_element_type=f32)
            for half in range(2):
                scores = both[half * 256:(half + 1) * 256]
                last = jnp.maximum(jnp.minimum(scores[:, r * 256:], limits[0]), limits[1])
                scores = jnp.concatenate([scores[:, :r * 256], last], axis=1) if r else last
                probs.append(jnp.exp(scores - jnp.max(scores, axis=1, keepdims=True)).astype(bf16))
            out = jnp.dot(jnp.concatenate(probs, axis=0), v, preferred_element_type=f32)
            outs = [out[half * 256:(half + 1) * 256, :128] / out[half * 256:(half + 1) * 256, 128:] for half in range(2)]
            ctx[unit, r * 256:n, lanes] = jnp.where(lane < 64, outs[0], outs[1]).astype(bf16)
        return carry

    def leave(r):
        return pltpu.make_async_copy(x.at[rows(r)], out_hbm.at[rows(r)], out_sem.at[r])

    def layer_body(layer, carry):
        base = layer * UNITS

        def project_in(half, width, start):
            cols = pl.ds(start, width)
            w = jnp.concatenate([blocks[base + 3 * half + kind, :, :, :, :, cols].reshape(1024, width) for kind in range(3)], axis=1)
            out = jnp.dot(a[...], w, preferred_element_type=f32)
            for kind in range(3):
                slot = 2 * kind + half
                piece = out[:, kind * width:(kind + 1) * width] + bias_rows[layer * 6 + slot, :, cols]
                qkv[slot, :, cols] = (piece * 0.125 if kind == 0 else piece).astype(bf16)

        caches = (pltpu.make_async_copy(keys, key_hbm.at[layer], key_sem),
                  pltpu.make_async_copy(values, value_hbm.at[layer], value_sem))

        def attend_pair(pair, carry):
            torus.poll('qkv', layer, pair)
            half, second = lax.div(pair, 2), lax.rem(pair, 2)

            @pl.when(layer == 0)
            def _():
                project_in(half, 128, pl.multiple_of(second * 128, 128))

            @pl.when((layer == 1) & (second == 0))
            def _():
                project_in(half, 256, 0)

            torus.poll('attn', layer, pair)
            attention(layer, pair, carry)
            return carry

        lax.fori_loop(0, 4, attend_pair, 0)

        def send_after(kind, r):
            @pl.when(r > 0)
            def _():
                exchange(layer, kind, r - 1).start()

        def project(r, carry):
            torus.poll('proj', layer, r)
            c = jnp.concatenate([ctx[0, rows(r)], ctx[1, rows(r)]], axis=1)
            w = jnp.concatenate([weight(base + 6), weight(base + 7)], axis=1)
            part[0, rows(r)] = lax.dot_general(c, w, NT, preferred_element_type=f32).astype(bf16)
            send_after(0, r)
            return carry

        lax.fori_loop(0, 4, project, 0)

        def turn(half, carry):
            keys[rows(half)] = qkv[2 + half].T
            values[rows(half)] = qkv[4 + half].T

            @pl.when(half == 0)
            def _():
                exchange(layer, 0, 3).start()
            return carry

        lax.fori_loop(0, 2, turn, 0)
        for cache in caches:
            cache.start()

        def second_norm(r, carry):
            torus.poll('mid', layer, r)
            total = residual(layer, 0, r, row_of(bout_ref, layer))
            a[rows(r)] = normalize(total, row_of(ln2s_ref, layer), row_of(ln2b_ref, layer))
            return carry

        lax.fori_loop(0, 4, second_norm, 0)

        def up_unit(j, carry):
            torus.poll('up', layer, j)
            cols = pl.ds(pl.multiple_of(j * 256, 256), 256)
            both = bup_ref[:, cols].astype(f32)
            bias = jnp.where(layer == 0, both[0:1], both[1:2])
            out = jnp.dot(a[...], weight(base + 8 + j), preferred_element_type=f32) + bias
            act[j] = gelu(out).astype(bf16)
            return carry

        lax.fori_loop(0, 8, up_unit, 0)

        def down_product(r, units):
            h = jnp.concatenate([act[j, rows(r)] for j in units], axis=1)
            w = jnp.concatenate([weight(base + 16 + j) for j in units], axis=1)
            return lax.dot_general(h, w, NT, preferred_element_type=f32)

        def down_next(r, carry):
            torus.poll('d1', layer, r)
            acc[rows(r)] = down_product(r, (0, 1, 2, 3, 4))
            return carry

        def down_last(r, carry):
            torus.poll('d2', layer, r)
            part[1, rows(r)] = (acc[rows(r)] + down_product(r, (5, 6, 7))).astype(bf16)
            send_after(1, r)
            return carry

        lax.fori_loop(0, 4, down_next, 0)
        lax.fori_loop(0, 4, down_last, 0)
        for cache in caches:
            cache.wait()
        exchange(layer, 1, 3).start()

        @pl.when(layer == 1)
        def _():
            for chunk in range(CHUNKS):
                for stage in range(STAGES):
                    if torus.used(chunk, stage):
                        torus.wait(send_sem, chunk, stage)

        def finish(r, carry):
            torus.poll('fin', layer, r)
            total = residual(layer, 1, r, row_of(bdown_ref, layer))

            @pl.when(layer == 0)
            def _():
                a[rows(r)] = normalize(total, ln1s_ref[1:2].astype(f32), ln1b_ref[1:2].astype(f32))

            @pl.when((layer == 1) & (r > 0))
            def _():
                leave(r - 1).start()
            return carry

        lax.fori_loop(0, 4, finish, 0)

        def sent(r, carry):
            exchange(layer, 0, r).wait_send()
            exchange(layer, 1, r).wait_send()
            return carry

        lax.fori_loop(0, 4, sent, 0)
        return carry

    lax.fori_loop(0, 2, layer_body, 0)
    leave(3).start()
    for r in range(4):
        leave(r).wait()


def run_layers(*operands):
    vmem, hbm = pl.BlockSpec(memory_space=pltpu.VMEM), pl.BlockSpec(memory_space=pl.ANY)
    bf16, dma = jnp.bfloat16, pltpu.SemaphoreType.DMA
    return pl.pallas_call(
        layers_kernel,
        out_shape=(jax.ShapeDtypeStruct((1024, 1024), bf16),) + (jax.ShapeDtypeStruct((2, 512, 1024), bf16),) * 2,
        in_specs=[hbm] + [vmem] * 12 + [hbm] * 2,
        out_specs=(hbm,) * 3,
        scratch_shapes=[
            pltpu.VMEM((2 * UNITS, 4, 4, 4, 16, 256), bf16),
            pltpu.VMEM((1024, 1024), bf16),
            pltpu.VMEM((1024, 1024), bf16),
            pltpu.VMEM((6, 1024, 256), bf16),
            pltpu.VMEM((2, 1024, 256), bf16),
            pltpu.VMEM((8, 1024, 256), bf16),
            pltpu.VMEM((1024, 1024), jnp.float32),
            pltpu.VMEM((2, 1024, 1024), bf16),
            pltpu.VMEM((2, 1024, 1024), bf16),
            pltpu.VMEM((1024, 128), bf16),
            pltpu.VMEM((2, 256, 256), jnp.float32),
            pltpu.VMEM((12, 1, 256), jnp.float32),
            pltpu.VMEM((512, 1024), bf16),
            pltpu.VMEM((512, 1024), bf16),
            dma((CHUNKS, STAGES)),
            dma((CHUNKS, STAGES)),
            dma((2, 2, 4)),
            dma((2, 2, 4)),
            dma,
            dma,
            dma,
            dma,
            dma((4,)),
        ],
        compiler_params=pltpu.CompilerParams(collective_id=0, has_side_effects=True, vmem_limit_bytes=58*2**20),
        name='two_layers',
    )(*operands)


PIECES = 4


def pass_kernel(*refs):
    sources, targets, (held, in_sem, out_sem) = refs[:3], refs[3:6], refs[6:]
    size = 1024 // PIECES
    views = [(k * PIECES + p, sources[k].at[p * size:(p + 1) * size], targets[k].at[p * size:(p + 1) * size])
             for p in range(PIECES) for k in range(3)]
    into = [pltpu.make_async_copy(src, held.at[n], in_sem.at[n]) for n, src, _ in views]
    out = [pltpu.make_async_copy(held.at[n], dst, out_sem.at[n]) for n, _, dst in views]
    for copy in into:
        copy.start()
    for first, second in zip(into, out):
        first.wait()
        second.start()
    for copy in out:
        copy.wait()


def pass_on(*arrays):
    shape = jax.ShapeDtypeStruct((1024, 1024), jnp.bfloat16)
    dma = pltpu.SemaphoreType.DMA
    return pl.pallas_call(
        pass_kernel,
        out_shape=(shape,) * 3,
        in_specs=[pl.BlockSpec(memory_space=pl.ANY)] * 3,
        out_specs=(pl.BlockSpec(memory_space=pl.ANY),) * 3,
        scratch_shapes=[pltpu.VMEM((3 * PIECES, 1024 // PIECES, 1024), jnp.bfloat16), dma((3 * PIECES,)), dma((3 * PIECES,))],
        name='pass_on',
    )(*arrays)


def solution(mesh):
    tp_size = mesh.shape['tp']
    batch_axes = ('dp', 'wg')

    def device_fn(hidden, attn_mask, ln1_scale, ln1_bias, w_qkv, b_qkv, w_out, b_out,
                  ln2_scale, ln2_bias, w_up, b_up, w_down, b_down):
        n_layers, _, local_heads, _, head_dim = w_qkv.shape
        slopes = np.zeros((tp_size, 128), np.float32)
        slopes[:, :3 * local_heads] = np.repeat(alibi_slopes(local_heads * tp_size).reshape(tp_size, local_heads), 3, axis=1)
        out, keys, values = run_layers(
            hidden.reshape(hidden.shape[1:]), attn_mask, slopes, ln1_scale, ln1_bias, ln2_scale, ln2_bias,
            b_qkv.transpose(0, 2, 1, 3), b_out, b_up, b_down, w_out.transpose(0, 1, 3, 2),
            w_qkv.transpose(0, 1, 3, 2, 4), w_up, w_down.transpose(0, 2, 1))
        out, keys, values = pass_on(out, keys.reshape(1024, 1024), values.reshape(1024, 1024))
        caches = [c.reshape(n_layers, 1, local_heads, head_dim, 1024).transpose(0, 1, 4, 2, 3) for c in (keys, values)]
        return out.reshape(hidden.shape), *caches

    replicated = P(None, None)
    in_specs = (P(batch_axes, None, None), P(batch_axes, None), replicated, replicated,
                P(None, 'wg', 'tp', None, None), P(None, 'tp', None, None), P(None, 'tp', None, 'wg'), replicated,
                replicated, replicated, P(None, 'wg', 'tp'), P(None, 'tp'), P(None, 'tp', 'wg'), replicated)
    cache_spec = P(None, batch_axes, None, 'tp', None)
    out_specs = (P(batch_axes, None, None), cache_spec, cache_spec)
    return jax.shard_map(device_fn, mesh=mesh, in_specs=in_specs, out_specs=out_specs, check_vma=False)
```

```python
import math
import jax
import jax.numpy as jnp
import numpy as np
from jax import lax
from jax.experimental import pallas as pl
from jax.experimental.pallas import tpu as pltpu
from jax.sharding import PartitionSpec as P

LN_EPS = 1e-5
GELU_A = math.sqrt(2.0 / math.pi)
GELU_B = 0.044715 * GELU_A
MESH = pl.DeviceIdType.MESH
UNITS = 24
HALVES = 4
CHUNKS = 18
DIRECT = (0, 1)
STAGES = 6
SCHEDULE = {
    'head': ((0, 0, ((0, 0), (1, 0), (2, 0), (3, 0), (4, 0), (5, 0), (6, 0), (7, 0), (8, 0), (9, 0), (10, 0), (11, 0), (12, 0), (13, 0), (14, 0), (15, 0), (16, 0), (17, 0))),),
    'norm': ((0, 3, ((2, 1), (0, 1), (0, 2), (3, 1), (4, 1), (5, 1), (1, 1), (1, 2))),),
    'qkv': ((0, 0, ((0, 3), (6, 1), (7, 1), (8, 1), (9, 1), (10, 1), (11, 1), (12, 1), (13, 1), (14, 1), (15, 1), (16, 1), (2, 2), (3, 2), (4, 2), (5, 2), (0, 4), (6, 2), (8, 2), (16, 2), (3, 3), (1, 3), (1, 4), (0, 5), (2, 3), (4, 3), (5, 3), (7, 2), (8, 3), (6, 3), (16, 3), (9, 2), (1, 5), (3, 4), (0, 6), (10, 2))), (0, 1, ((1, 6),)), (0, 2, ((2, 5), (4, 5), (5, 5), (6, 4), (2, 6))), (0, 3, ((3, 6),)), (1, 0, ((10, 6), (11, 5))), (1, 2, ((13, 5), (11, 6)))),
    'attn': ((0, 0, ((2, 4), (4, 4))), (0, 1, ((3, 5), (5, 4))), (0, 2, ((7, 3), (8, 4))), (0, 3, ((9, 3), (10, 3), (11, 2), (12, 2), (13, 2))), (1, 0, ((14, 3), (15, 3), (16, 5))), (1, 1, ((12, 5), (17, 2))), (1, 2, ((14, 4),)), (1, 3, ((15, 4),))),
    'proj': ((0, 0, ((4, 6),)), (0, 1, ((6, 5),)), (1, 0, ((12, 6),)), (1, 3, ((17, 3),))),
    'mid': ((0, 0, ((7, 4),)), (0, 2, ((8, 5),)), (1, 1, ((14, 5),))),
    'up': ((0, 0, ((9, 4),)), (0, 1, ((5, 6),)), (0, 3, ((10, 4),)), (0, 4, ((6, 6),)), (0, 6, ((7, 5),)), (0, 7, ((9, 5), (10, 5), (11, 3), (12, 3), (13, 3), (14, 2), (7, 6), (15, 2))), (1, 0, ((15, 5), (17, 4))), (1, 1, ((13, 6),)), (1, 4, ((14, 6),)), (1, 7, ((15, 6),))),
    'd1': ((0, 0, ((8, 6), (16, 4))), (0, 2, ((17, 1), (11, 4))), (1, 0, ((16, 6), (17, 5)))),
    'd2': ((0, 0, ((9, 6),)), (0, 2, ((12, 4),)), (1, 0, ((17, 6),))),
    'fin': ((0, 0, ((13, 4),)),),
}
NT = (((1,), (1,)), ((), ()))
ORDERS = (('x', 'y', 'z'), ('y', 'z', 'x'), ('z', 'x', 'y'))


def alibi_slopes(n_heads):
    closest = 2 ** int(math.floor(math.log2(n_heads)))
    slope_base = 2.0 ** (-8.0 / closest)
    slope_list = [slope_base ** (i + 1) for i in range(closest)]
    extra_base = 2.0 ** (-4.0 / closest)
    slope_list = slope_list + [extra_base ** (2 * i + 1) for i in range(n_heads - closest)]
    return np.array(slope_list, dtype=np.float32)


class Torus:
    def __init__(self, blocks, send_sem, recv_sem):
        self.blocks, self.send_sem, self.recv_sem = blocks, send_sem, recv_sem
        me = lax.axis_index('wg')
        self.pos = {'z': lax.div(me, 16), 'y': lax.rem(lax.div(me, 4), 4), 'x': lax.rem(me, 4)}
        self.next = {ax: lax.rem(p + 1, 4) for ax, p in self.pos.items()}
        self.prev = {ax: lax.rem(p + 3, 4) for ax, p in self.pos.items()}
        self.right = {ax: self.device({**self.pos, ax: self.next[ax]}) for ax in 'zyx'}
        self.across = {ax: self.device({**self.pos, ax: lax.rem(self.pos[ax] + 2, 4)}) for ax in 'zyx'}
        self.left = {ax: self.device({**self.pos, ax: self.prev[ax]}) for ax in 'zyx'}

    @staticmethod
    def device(pos):
        return pos['z'] * 16 + pos['y'] * 4 + pos['x']

    def view(self, unit, where, cols=slice(0, 256)):
        return self.blocks.at[unit, where['z'], where['y'], where['x'], :, cols]

    def greet(self):
        sem = pltpu.get_barrier_semaphore()
        for ax in 'zyx':
            for dev in (self.left[ax], self.right[ax], self.across[ax]):
                pl.semaphore_signal(sem, inc=1, device_id={'wg': dev}, device_id_type=MESH)
        pl.semaphore_signal(sem, inc=1, device_id={'tp': 1 - lax.axis_index('tp')}, device_id_type=MESH)

    def meet(self):
        pl.semaphore_wait(pltpu.get_barrier_semaphore(), 10)

    def part(self, chunk):
        if chunk < HALVES:
            return 3 * (chunk // 2), (chunk % 2) * 128, 128
        return 3 * (chunk - HALVES // 2), 0, 256

    def sends(self, chunk, stage):
        every, low, high = slice(None), slice(0, 2), slice(2, 4)
        first, start, width = self.part(chunk)
        cols = slice(start, start + width)
        out = []
        for color, (a, b, c) in enumerate(ORDERS):
            unit = first + color
            if stage in (0, 2, 4):
                axis = (a, b, c)[stage // 2]
                held = {**self.pos, **{ax: every for ax in (a, b)[:stage // 2]}}
                ref = self.view(unit, held, cols)
                out += [(ref, self.right[axis]), (ref, self.left[axis])]
                if chunk in DIRECT and stage < 4:
                    out.append((ref, self.across[axis]))
            elif stage == 1:
                ahead, back = {**self.pos, a: self.prev[a]}, {**self.pos, a: self.next[a]}
                if width == 256:
                    out += [(self.view(unit, ahead, slice(0, 128)), self.right[a]), (self.view(unit, back, slice(128, 256)), self.left[a])]
                elif chunk % 2 == 0:
                    out.append((self.view(unit, ahead, cols), self.right[a]))
                else:
                    out.append((self.view(unit, back, cols), self.left[a]))
            elif stage == 3:
                out += [(self.view(unit, {a: low, b: self.prev[b], c: self.pos[c]}, cols), self.right[b]),
                        (self.view(unit, {a: high, b: self.next[b], c: self.pos[c]}, cols), self.left[b])]
            else:
                slow, fast = (a, b) if 'zyx'.index(a) < 'zyx'.index(b) else (b, a)
                out += [(self.view(unit, {slow: low, fast: every, c: self.prev[c]}, cols), self.right[c]),
                        (self.view(unit, {slow: high, fast: every, c: self.next[c]}, cols), self.left[c])]
        return out

    def start(self, chunk, stage):
        for ref, dev in self.sends(chunk, stage):
            pltpu.make_async_remote_copy(
                src_ref=ref, dst_ref=ref, send_sem=self.send_sem.at[chunk, stage], recv_sem=self.recv_sem.at[chunk, stage],
                device_id={'wg': dev}, device_id_type=MESH).start()

    def wait(self, sem, chunk, stage):
        every, three = slice(None), slice(0, 3)
        peers = three if chunk in DIRECT else slice(0, 2)
        where = ((0, 0, peers), (0, 0, 0), (0, peers, every), (0, 0, every), (slice(0, 2), every, every), (0, every, every))[stage]
        size = self.blocks.at[(three,) + where + (every, slice(0, self.part(chunk)[2]))]
        pltpu.make_async_copy(size, size, sem.at[chunk, stage]).wait()

    def used(self, chunk, stage):
        return stage < STAGES and not (chunk in DIRECT and stage in (1, 3))

    def step(self, chunk, stage):
        before = [n for n in range(stage) if self.used(chunk, n)]
        if stage < STAGES and not self.used(chunk, stage):
            return
        if before:
            self.wait(self.recv_sem, chunk, before[-1])
        if stage < STAGES:
            self.start(chunk, stage)

    def poll(self, piece, layer, index):
        for at_layer, at_index, due in SCHEDULE.get(piece, ()):
            @pl.when((layer == at_layer) & (index == at_index))
            def _():
                for chunk, stage in due:
                    self.step(chunk, stage)


def normalize(values, scale, shift):
    mean = jnp.mean(values, axis=1, keepdims=True)
    centered = values - mean
    variance = jnp.mean(centered * centered, axis=1, keepdims=True)
    return (centered * lax.rsqrt(variance + LN_EPS) * scale + shift).astype(jnp.bfloat16)


def gelu(h):
    half = 0.5 * h
    return half + half * jnp.tanh(h * (GELU_A + GELU_B * (h * h)))


def rows(r, size=256):
    return pl.ds(pl.multiple_of(r * size, size), size)


def layers_kernel(x_hbm, mask_ref, slope_ref, ln1s_ref, ln1b_ref, ln2s_ref, ln2b_ref, bqkv_ref, bout_ref, bup_ref, bdown_ref,
                  wout_ref, wqkv_ref, wup_hbm, wdown_hbm, out_hbm, key_hbm, value_hbm,
                  blocks, x, a, qkv, ctx, act, acc, part, other, bias_cols, limits, bias_rows, keys, values,
                  send_sem, recv_sem, part_send, part_recv, own_sem, x_sem, key_sem, value_sem, out_sem):
    f32, bf16 = jnp.float32, jnp.bfloat16
    torus = Torus(blocks, send_sem, recv_sem)
    partner = {'tp': 1 - lax.axis_index('tp')}
    mine = (torus.pos['z'], torus.pos['y'], torus.pos['x'])
    own = []
    torus.greet()
    for layer in range(2):
        for first, weights in ((8, wup_hbm), (16, wdown_hbm)):
            own += [pltpu.make_async_copy(weights.at[layer, :, j * 256:(j + 1) * 256],
                                          blocks.at[(layer * UNITS + first + j,) + mine], own_sem) for j in range(8)]
    for copy in own:
        copy.start()
    x_in = pltpu.make_async_copy(x_hbm, x, x_sem)
    x_in.start()
    for layer in range(2):
        flat = jnp.concatenate([wout_ref[layer, head] for head in range(8)], axis=1)
        for j in range(2):
            blocks[(layer * UNITS + 6 + j,) + mine] = flat[:, j * 256:(j + 1) * 256]
    for layer in range(2):
        for half in range(2):
            for kind in range(3):
                heads = [wqkv_ref[layer, :, kind, h, :] for h in range(4 * half, 4 * half + 4)]
                blocks[(layer * UNITS + 3 * half + kind,) + mine] = jnp.concatenate(heads, axis=1)
    torus.meet()
    whole = blocks.at[0:32, 0, 0, 0]
    pltpu.make_async_copy(whole, whole, own_sem).wait()
    zero = jnp.int32(0)
    torus.poll('head', zero, zero)

    def row_of(ref, layer):
        both = ref[...].astype(f32)
        return jnp.where(layer == 0, both[0:1], both[1:2])

    def weight(unit):
        return blocks[unit].reshape(1024, 256)

    real = jnp.sum(mask_ref[...].astype(f32), axis=1, keepdims=True)
    key = lax.broadcasted_iota(jnp.int32, (1024, 128), 0).astype(f32)
    lane = lax.broadcasted_iota(jnp.int32, (1024, 128), 1)
    place = key - (1024.0 - real)
    slope = jnp.where(lax.axis_index('tp') == 0, slope_ref[0:1], slope_ref[1:2])
    key_bias = jnp.where(place >= 0.0, place * slope, -1e30)
    first = key_bias.astype(bf16)
    rest = key_bias - first.astype(f32)
    second = rest.astype(bf16)
    third = (rest - second.astype(f32)).astype(bf16)
    which = lax.rem(lane, 3)
    split = jnp.where(which == 0, first.astype(f32), jnp.where(which == 1, second.astype(f32), third.astype(f32)))
    bias_cols[...] = jnp.where(lane < 24, split, 0.0).astype(bf16)
    row = lax.broadcasted_iota(jnp.int32, (256, 256), 0)
    col = lax.broadcasted_iota(jnp.int32, (256, 256), 1)
    limits[0] = jnp.where(col <= row, 3e38, -1e30)
    limits[1] = jnp.where(col == row, -1e29, -3e38)

    for layer in range(2):
        for kind in range(3):
            heads = bqkv_ref[layer, kind].astype(f32)
            for j in range(2):
                bias_rows[layer * 6 + kind * 2 + j] = jnp.concatenate([heads[h:h + 1] for h in range(4 * j, 4 * j + 4)], axis=1)

    x_in.wait()

    def first_norm(r, carry):
        torus.poll('norm', zero, r)
        a[rows(r)] = normalize(x[rows(r)].astype(f32), ln1s_ref[0:1].astype(f32), ln1b_ref[0:1].astype(f32))
        return carry

    lax.fori_loop(0, 4, first_norm, 0)

    def exchange(layer, kind, r):
        view = lambda ref: ref.at[kind, rows(r)]
        return pltpu.make_async_remote_copy(
            src_ref=view(part), dst_ref=view(other), send_sem=part_send.at[layer, kind, r], recv_sem=part_recv.at[layer, kind, r],
            device_id=partner, device_id_type=MESH)

    def residual(layer, kind, r, bias):
        exchange(layer, kind, r).wait_recv()
        branch = part[kind, rows(r)].astype(f32) + other[kind, rows(r)].astype(f32)
        total = (x[rows(r)].astype(f32) + branch + bias).astype(bf16)
        x[rows(r)] = total
        return total.astype(f32)

    def attention(layer, pair, carry):
        unit, lanes = lax.div(pair, 2), pl.ds(pl.multiple_of(lax.rem(pair, 2) * 128, 128), 128)
        lane = lax.broadcasted_iota(jnp.int32, (256, 128), 1)
        def score(r):
            n = (r + 1) * 256
            q = qkv[unit, r * 256:n, lanes]
            k = jnp.concatenate([qkv[2 + unit, 0:n, lanes], bias_cols[0:n]], axis=1)
            queries = []
            for half in range(2):
                mine = (lane < 64) if half == 0 else (lane >= 64)
                head = 2 * pair + half
                pick = ((lane >= 3 * head) & (lane < 3 * head + 3)).astype(bf16)
                queries.append(jnp.concatenate([jnp.where(mine, q, jnp.zeros_like(q)), pick], axis=1))
            return lax.dot_general(jnp.concatenate(queries, axis=0), k, NT, preferred_element_type=f32)

        def weigh(r, both):
            probs = []
            for half in range(2):
                scores = both[half * 256:(half + 1) * 256]
                last = jnp.maximum(jnp.minimum(scores[:, r * 256:], limits[0]), limits[1])
                scores = jnp.concatenate([scores[:, :r * 256], last], axis=1) if r else last
                probs.append(jnp.exp(scores - jnp.max(scores, axis=1, keepdims=True)).astype(bf16))
            return jnp.concatenate(probs, axis=0)

        def mix(r, probs):
            n = (r + 1) * 256
            v = jnp.concatenate([qkv[4 + unit, 0:n, lanes], jnp.ones((n, 128), bf16)], axis=1)
            out = jnp.dot(probs, v, preferred_element_type=f32)
            outs = [out[half * 256:(half + 1) * 256, :128] / out[half * 256:(half + 1) * 256, 128:] for half in range(2)]
            ctx[unit, r * 256:n, lanes] = jnp.where(lane < 64, outs[0], outs[1]).astype(bf16)

        order = (3, 2, 1, 0)
        scores, probs = {3: score(3)}, {}
        for n, r in enumerate(order):
            if n < 3:
                scores[r - 1] = score(r - 1)
            probs[r] = weigh(r, scores.pop(r))
            if n > 0:
                mix(r + 1, probs.pop(r + 1))
        mix(0, probs.pop(0))
        return carry

    def leave(r):
        return pltpu.make_async_copy(x.at[rows(r)], out_hbm.at[rows(r)], out_sem.at[r])

    def layer_body(layer, carry):
        base = layer * UNITS

        def project_in(half, width, start):
            cols = pl.ds(start, width)
            w = jnp.concatenate([blocks[base + 3 * half + kind, :, :, :, :, cols].reshape(1024, width) for kind in range(3)], axis=1)
            out = jnp.dot(a[...], w, preferred_element_type=f32)
            for kind in range(3):
                slot = 2 * kind + half
                piece = out[:, kind * width:(kind + 1) * width] + bias_rows[layer * 6 + slot, :, cols]
                qkv[slot, :, cols] = (piece * 0.125 if kind == 0 else piece).astype(bf16)

        caches = (pltpu.make_async_copy(keys, key_hbm.at[layer], key_sem),
                  pltpu.make_async_copy(values, value_hbm.at[layer], value_sem))

        def attend_pair(pair, carry):
            torus.poll('qkv', layer, pair)
            half, second = lax.div(pair, 2), lax.rem(pair, 2)

            @pl.when(layer == 0)
            def _():
                project_in(half, 128, pl.multiple_of(second * 128, 128))

            @pl.when((layer == 1) & (second == 0))
            def _():
                project_in(half, 256, 0)

            torus.poll('attn', layer, pair)
            attention(layer, pair, carry)
            return carry

        lax.fori_loop(0, 4, attend_pair, 0)

        def send_after(kind, r):
            @pl.when(r > 0)
            def _():
                exchange(layer, kind, r - 1).start()

        def project(r, carry):
            torus.poll('proj', layer, r)
            c = jnp.concatenate([ctx[0, rows(r)], ctx[1, rows(r)]], axis=1)
            w = jnp.concatenate([weight(base + 6), weight(base + 7)], axis=1)
            part[0, rows(r)] = lax.dot_general(c, w, NT, preferred_element_type=f32).astype(bf16)
            send_after(0, r)
            return carry

        lax.fori_loop(0, 4, project, 0)

        def turn(half, carry):
            keys[rows(half)] = qkv[2 + half].T
            values[rows(half)] = qkv[4 + half].T

            @pl.when(half == 0)
            def _():
                exchange(layer, 0, 3).start()
            return carry

        lax.fori_loop(0, 2, turn, 0)
        for cache in caches:
            cache.start()

        def second_norm(r, carry):
            torus.poll('mid', layer, r)
            total = residual(layer, 0, r, row_of(bout_ref, layer))
            a[rows(r)] = normalize(total, row_of(ln2s_ref, layer), row_of(ln2b_ref, layer))
            return carry

        lax.fori_loop(0, 4, second_norm, 0)

        def up_unit(j, carry):
            torus.poll('up', layer, j)
            cols = pl.ds(pl.multiple_of(j * 256, 256), 256)
            both = bup_ref[:, cols].astype(f32)
            bias = jnp.where(layer == 0, both[0:1], both[1:2])
            out = jnp.dot(a[...], weight(base + 8 + j), preferred_element_type=f32) + bias
            act[j] = gelu(out).astype(bf16)
            return carry

        lax.fori_loop(0, 8, up_unit, 0)

        def down_product(r, units):
            h = jnp.concatenate([act[j, rows(r)] for j in units], axis=1)
            w = jnp.concatenate([weight(base + 16 + j) for j in units], axis=1)
            return lax.dot_general(h, w, NT, preferred_element_type=f32)

        def down_next(r, carry):
            torus.poll('d1', layer, r)
            acc[rows(r)] = down_product(r, (0, 1, 2, 3, 4))
            return carry

        def down_last(r, carry):
            torus.poll('d2', layer, r)
            part[1, rows(r)] = (acc[rows(r)] + down_product(r, (5, 6, 7))).astype(bf16)
            send_after(1, r)
            return carry

        lax.fori_loop(0, 4, down_next, 0)
        lax.fori_loop(0, 4, down_last, 0)
        for cache in caches:
            cache.wait()
        exchange(layer, 1, 3).start()

        @pl.when(layer == 1)
        def _():
            for chunk in range(CHUNKS):
                for stage in range(STAGES):
                    if torus.used(chunk, stage):
                        torus.wait(send_sem, chunk, stage)

        def finish(r, carry):
            torus.poll('fin', layer, r)
            total = residual(layer, 1, r, row_of(bdown_ref, layer))

            @pl.when(layer == 0)
            def _():
                a[rows(r)] = normalize(total, ln1s_ref[1:2].astype(f32), ln1b_ref[1:2].astype(f32))

            @pl.when((layer == 1) & (r > 0))
            def _():
                leave(r - 1).start()
            return carry

        lax.fori_loop(0, 4, finish, 0)

        def sent(r, carry):
            exchange(layer, 0, r).wait_send()
            exchange(layer, 1, r).wait_send()
            return carry

        lax.fori_loop(0, 4, sent, 0)
        return carry

    lax.fori_loop(0, 2, layer_body, 0)
    leave(3).start()
    for r in range(4):
        leave(r).wait()


def run_layers(*operands):
    vmem, hbm = pl.BlockSpec(memory_space=pltpu.VMEM), pl.BlockSpec(memory_space=pl.ANY)
    bf16, dma = jnp.bfloat16, pltpu.SemaphoreType.DMA
    return pl.pallas_call(
        layers_kernel,
        out_shape=(jax.ShapeDtypeStruct((1024, 1024), bf16),) + (jax.ShapeDtypeStruct((2, 512, 1024), bf16),) * 2,
        in_specs=[hbm] + [vmem] * 12 + [hbm] * 2,
        out_specs=(hbm,) * 3,
        scratch_shapes=[
            pltpu.VMEM((2 * UNITS, 4, 4, 4, 16, 256), bf16),
            pltpu.VMEM((1024, 1024), bf16),
            pltpu.VMEM((1024, 1024), bf16),
            pltpu.VMEM((6, 1024, 256), bf16),
            pltpu.VMEM((2, 1024, 256), bf16),
            pltpu.VMEM((8, 1024, 256), bf16),
            pltpu.VMEM((1024, 1024), jnp.float32),
            pltpu.VMEM((2, 1024, 1024), bf16),
            pltpu.VMEM((2, 1024, 1024), bf16),
            pltpu.VMEM((1024, 128), bf16),
            pltpu.VMEM((2, 256, 256), jnp.float32),
            pltpu.VMEM((12, 1, 256), jnp.float32),
            pltpu.VMEM((512, 1024), bf16),
            pltpu.VMEM((512, 1024), bf16),
            dma((CHUNKS, STAGES)),
            dma((CHUNKS, STAGES)),
            dma((2, 2, 4)),
            dma((2, 2, 4)),
            dma,
            dma,
            dma,
            dma,
            dma((4,)),
        ],
        compiler_params=pltpu.CompilerParams(collective_id=0, has_side_effects=True, vmem_limit_bytes=67043328),
        name='two_layers',
    )(*operands)


PIECES = 4


def pass_kernel(*refs):
    sources, targets, (held, in_sem, out_sem) = refs[:3], refs[3:6], refs[6:]
    size = 1024 // PIECES
    views = [(k * PIECES + p, sources[k].at[p * size:(p + 1) * size], targets[k].at[p * size:(p + 1) * size])
             for p in range(PIECES) for k in range(3)]
    into = [pltpu.make_async_copy(src, held.at[n], in_sem.at[n]) for n, src, _ in views]
    out = [pltpu.make_async_copy(held.at[n], dst, out_sem.at[n]) for n, _, dst in views]
    for copy in into:
        copy.start()
    for first, second in zip(into, out):
        first.wait()
        second.start()
    for copy in out:
        copy.wait()


def pass_on(*arrays):
    shape = jax.ShapeDtypeStruct((1024, 1024), jnp.bfloat16)
    dma = pltpu.SemaphoreType.DMA
    return pl.pallas_call(
        pass_kernel,
        out_shape=(shape,) * 3,
        in_specs=[pl.BlockSpec(memory_space=pl.ANY)] * 3,
        out_specs=(pl.BlockSpec(memory_space=pl.ANY),) * 3,
        scratch_shapes=[pltpu.VMEM((3 * PIECES, 1024 // PIECES, 1024), jnp.bfloat16), dma((3 * PIECES,)), dma((3 * PIECES,))],
        name='pass_on',
    )(*arrays)


def solution(mesh):
    tp_size = mesh.shape['tp']
    batch_axes = ('dp', 'wg')

    def device_fn(hidden, attn_mask, ln1_scale, ln1_bias, w_qkv, b_qkv, w_out, b_out,
                  ln2_scale, ln2_bias, w_up, b_up, w_down, b_down):
        n_layers, _, local_heads, _, head_dim = w_qkv.shape
        slopes = np.zeros((tp_size, 128), np.float32)
        slopes[:, :3 * local_heads] = np.repeat(alibi_slopes(local_heads * tp_size).reshape(tp_size, local_heads), 3, axis=1)
        out, keys, values = run_layers(
            hidden.reshape(hidden.shape[1:]), attn_mask, slopes, ln1_scale, ln1_bias, ln2_scale, ln2_bias,
            b_qkv.transpose(0, 2, 1, 3), b_out, b_up, b_down, w_out.transpose(0, 1, 3, 2),
            w_qkv.transpose(0, 1, 3, 2, 4), w_up, w_down.transpose(0, 2, 1))
        out, keys, values = pass_on(out, keys.reshape(1024, 1024), values.reshape(1024, 1024))
        caches = [c.reshape(n_layers, 1, local_heads, head_dim, 1024).transpose(0, 1, 4, 2, 3) for c in (keys, values)]
        return out.reshape(hidden.shape), *caches

    replicated = P(None, None)
    in_specs = (P(batch_axes, None, None), P(batch_axes, None), replicated, replicated,
                P(None, 'wg', 'tp', None, None), P(None, 'tp', None, None), P(None, 'tp', None, 'wg'), replicated,
                replicated, replicated, P(None, 'wg', 'tp'), P(None, 'tp'), P(None, 'tp', 'wg'), replicated)
    cache_spec = P(None, batch_axes, None, 'tp', None)
    out_specs = (P(batch_axes, None, None), cache_spec, cache_spec)
    return jax.shard_map(device_fn, mesh=mesh, in_specs=in_specs, out_specs=out_specs, check_vma=False)
```
